16 devices in a mesh: dp: 4 (over z, y), dap: 4 (over x, core).
Axes of the slice: x: 2, y: 2, z: 2, core: 2. Of those that a mesh axis runs over, the one named last changes fastest.
Arguments:
- z_pair: bfloat16 [4, 256, 256, 128], P('dp', 'dap')
- pair_mask: int32 [4, 256, 256], P('dp', 'dap')
- dz_out: bfloat16 [4, 256, 256, 128], P('dp', 'dap')
- ln_in: bfloat16 [2, 2, 128], replicated
- w_proj: bfloat16 [2, 128, 640], replicated
- b_proj: bfloat16 [2, 640], replicated
- ln_mid: bfloat16 [2, 2, 128], replicated
- w_out: bfloat16 [2, 128, 128], replicated
- b_out: bfloat16 [2, 128], replicated
Outputs:
- output 1: bfloat16 [4, 256, 256, 128], P('dp', 'dap')
- output 2: bfloat16 [4, 256, 256, 128], P('dp', 'dap')
- output 3: float32 [2, 2, 128], replicated
- output 4: float32 [2, 128, 640], replicated
- output 5: float32 [2, 640], replicated
- output 6: float32 [2, 2, 128], replicated
- output 7: float32 [2, 128, 128], replicated
- output 8: float32 [2, 128], replicated
All inputs are finite; a program needn't handle non-finite values.
Results may differ from the reference program's by a relative error of at most 0.01347.
Values are sent between devices in bfloat16 or wider.
A program may use at most 1 GiB of HBM per device.

```python
import jax
import jax.numpy as jnp
from jax import lax

PROTEINS = 4
N_RES = 256
C_Z = 128
C_HID = 128
LN_EPS = 1e-5


def layer_norm(values, ln_gain, ln_bias):
    mean_val = jnp.mean(values, axis=-1, keepdims=True)
    centered = values - mean_val
    variance = jnp.mean(centered * centered, axis=-1, keepdims=True)
    return centered * lax.rsqrt(variance + LN_EPS) * ln_gain + ln_bias


def to_bf16(values):
    return values.astype(jnp.bfloat16).astype(jnp.float32)


def tri_block(z_in, mask_f, weights, incoming):
    ln_in, w_proj, b_proj, ln_mid, w_out, b_out = weights
    z_f32 = z_in.astype(jnp.float32)
    z_hat = to_bf16(layer_norm(z_f32, ln_in[0], ln_in[1]))
    proj_all = jnp.dot(z_hat, w_proj) + b_proj
    a_side = to_bf16(jax.nn.sigmoid(proj_all[..., :C_HID]) * proj_all[..., C_HID:2 * C_HID] * mask_f)
    b_side = to_bf16(jax.nn.sigmoid(proj_all[..., 2 * C_HID:3 * C_HID]) * proj_all[..., 3 * C_HID:4 * C_HID] * mask_f)
    g_side = jax.nn.sigmoid(proj_all[..., 4 * C_HID:])
    if incoming:
        tri_x = jnp.einsum("kic,kjc->ijc", a_side, b_side)
    else:
        tri_x = jnp.einsum("ikc,jkc->ijc", a_side, b_side)
    x_hat = to_bf16(layer_norm(tri_x, ln_mid[0], ln_mid[1]))
    update = jnp.dot(x_hat, w_out) + b_out
    return (z_f32 + g_side * update).astype(jnp.bfloat16)


def protein_grads(z_one, mask_one, dz_one, weights_all):
    mask_f = mask_one.astype(jnp.float32)[:, :, None]

    def forward(z_in, weights):
        first_set = tuple(weight_arr[0] for weight_arr in weights)
        second_set = tuple(weight_arr[1] for weight_arr in weights)
        z_mid = tri_block(z_in, mask_f, first_set, False)
        return tri_block(z_mid, mask_f, second_set, True)

    z_new, pull_back = jax.vjp(forward, z_one, weights_all)
    dz_in, d_weights = pull_back(dz_one)
    return z_new, dz_in, d_weights


def setup_inputs(seed: int = 0) -> dict:
    key_list = jax.random.split(jax.random.key(seed), 12)
    pair_shape = (PROTEINS, N_RES, N_RES, C_Z)
    proj_width = 4 * C_HID + C_Z
    z_pair = jax.random.normal(key_list[0], pair_shape, jnp.float32).astype(jnp.bfloat16)
    lengths = jax.random.randint(key_list[1], (PROTEINS,), N_RES // 2, N_RES + 1)
    positions = jnp.arange(N_RES)
    valid_res = positions[None, :] < lengths[:, None]
    pair_mask = (valid_res[:, :, None] & valid_res[:, None, :]).astype(jnp.int32)
    dz_out = jax.random.normal(key_list[2], pair_shape, jnp.float32).astype(jnp.bfloat16)
    ln_in = jnp.stack([1.0 + 0.3 * jax.random.normal(key_list[3], (2, C_Z), jnp.float32), 0.3 * jax.random.normal(key_list[4], (2, C_Z), jnp.float32)], axis=1).astype(jnp.bfloat16)
    w_proj = (jax.random.normal(key_list[5], (2, C_Z, proj_width), jnp.float32) * C_Z ** -0.5).astype(jnp.bfloat16)
    b_proj = (0.5 * jax.random.normal(key_list[6], (2, proj_width), jnp.float32)).astype(jnp.bfloat16)
    ln_mid = jnp.stack([1.0 + 0.3 * jax.random.normal(key_list[7], (2, C_HID), jnp.float32), 0.3 * jax.random.normal(key_list[8], (2, C_HID), jnp.float32)], axis=1).astype(jnp.bfloat16)
    w_out = (jax.random.normal(key_list[9], (2, C_HID, C_Z), jnp.float32) * C_HID ** -0.5).astype(jnp.bfloat16)
    b_out = (0.5 * jax.random.normal(key_list[10], (2, C_Z), jnp.float32)).astype(jnp.bfloat16)
    return {"z_pair": z_pair, "pair_mask": pair_mask, "dz_out": dz_out, "ln_in": ln_in, "w_proj": w_proj, "b_proj": b_proj, "ln_mid": ln_mid, "w_out": w_out, "b_out": b_out}


def reference(z_pair, pair_mask, dz_out, ln_in, w_proj, b_proj, ln_mid, w_out, b_out):
    weights_all = (ln_in.astype(jnp.float32), w_proj.astype(jnp.float32), b_proj.astype(jnp.float32), ln_mid.astype(jnp.float32), w_out.astype(jnp.float32), b_out.astype(jnp.float32))

    def per_protein(operands):
        z_one, mask_one, dz_one = operands
        return protein_grads(z_one, mask_one, dz_one, weights_all)

    z_new, dz_in, d_weights = lax.map(per_protein, (z_pair, pair_mask, dz_out))
    d_ln_in, d_w_proj, d_b_proj, d_ln_mid, d_w_out, d_b_out = d_weights
    return (z_new, dz_in, jnp.sum(d_ln_in, axis=0), jnp.sum(d_w_proj, axis=0), jnp.sum(d_b_proj, axis=0), jnp.sum(d_ln_mid, axis=0), jnp.sum(d_w_out, axis=0), jnp.sum(d_b_out, axis=0))
```

```python
import functools
import jax
import jax.numpy as jnp
from jax import lax
from jax.experimental import pallas as pl
from jax.experimental.pallas import tpu as pltpu
from jax.sharding import PartitionSpec as P

LN_EPS = 1e-5
RB = 16
SP = 17
UN = 4
F32 = jnp.float32
BF16 = jnp.bfloat16
C = 128
N = 256
QUAD = [[0, 2, 1, 3]]
SWAP_X = [(0, 2), (2, 0), (1, 3), (3, 1)]


def dot(a, b):
    return lax.dot_general(a, b, (((1,), (0,)), ((), ())), preferred_element_type=F32)


def dot_t(a, b):
    return dot(a, jnp.transpose(b))


def sig(v):
    return 0.5 * jnp.tanh(0.5 * v) + 0.5


def norm(v):
    mu = jnp.mean(v, axis=0, keepdims=True)
    vc = v - mu
    rstd = lax.rsqrt(jnp.mean(vc * vc, axis=0, keepdims=True) + LN_EPS)
    return vc * rstd, rstd


def norm_bwd(d_hat, vn, rstd, gain):
    dn = d_hat * gain
    m1 = jnp.mean(dn, axis=0, keepdims=True)
    m2 = jnp.mean(dn * vn, axis=0, keepdims=True)
    return rstd * (dn - m1 - vn * m2)


def perm_cols(t):
    return jnp.concatenate([t[0:64], t[128:192], t[64:128], t[192:256]], axis=0)


def load_t(ref, r):
    return jnp.transpose(perm_cols(ref[r])).astype(F32)


def store_t(ref, r, val):
    t = perm_cols(jnp.transpose(val)).astype(BF16)
    ref[r] = t


def put_row(scr, r, val):
    for h in range(2):
        scr[h, pl.ds(r, C, stride=SP), :] = val[:, h * 128:(h + 1) * 128]


def get_row(scr, r):
    return jnp.concatenate([scr[h, pl.ds(r, C, stride=SP), :] for h in range(2)], axis=1)


def pack(scr, out_ref):
    def body(i, _):
        c0 = i * 8
        for k in range(8):
            for h in range(2):
                out_ref[c0 + k, :, h * 128:(h + 1) * 128] = scr[h, pl.ds((c0 + k) * SP, RB), :].astype(out_ref.dtype)
        return 0
    lax.fori_loop(0, C // 8, body, 0)


def unpack(in_ref, scr):
    def body(i, _):
        c0 = i * 8
        for k in range(8):
            for h in range(2):
                scr[h, pl.ds((c0 + k) * SP, RB), :] = in_ref[c0 + k, :, h * 128:(h + 1) * 128].astype(F32)
        return 0
    lax.fori_loop(0, C // 8, body, 0)


def gates(zh, m, wt, bp, scr_a, scr_b, r):
    pa = dot(wt[0:256, :], zh)
    put_row(scr_a, r, sig(pa[0:128] + bp[0]) * (pa[128:256] + bp[1]) * m)
    pb = dot(wt[256:512, :], zh)
    put_row(scr_b, r, sig(pb[0:128] + bp[2]) * (pb[128:256] + bp[3]) * m)


CHUNKS = ((0, 640, (0, 1, 2, 3)), (640, 512, (0, 2, 3, 1)), (1152, 512, (0, 3, 1, 2)))
GROWS = 1664


def coords():
    return lax.axis_index("dp"), lax.axis_index("dap")


def partner(k):
    dp, dap = coords()
    if k < 2:
        bit = lax.rem(dap // (1 << k), 2)
        return bit, (dp, dap + (1 << k) * (1 - 2 * bit))
    bit = lax.rem(dp // (1 << (k - 2)), 2)
    return bit, (dp + (1 << (k - 2)) * (1 - 2 * bit), dap)


def greet(keys):
    barrier = pltpu.get_barrier_semaphore()
    for k in keys:
        pl.semaphore_signal(barrier, inc=1, device_id=partner(k)[1], device_id_type=pl.DeviceIdType.MESH)
    pl.semaphore_wait(barrier, len(keys))


def remote(src, dst, send, recv, k):
    return pltpu.make_async_remote_copy(src_ref=src, dst_ref=dst, send_sem=send, recv_sem=recv, device_id=partner(k)[1], device_id_type=pl.DeviceIdType.MESH)


def rb(i):
    return lax.rem(i + 4 * partner(1)[0], 8)


def first4(i):
    return lax.min(i, 3)


def pair_parts(step, st, out, split):
    bit = partner(0)[0]
    slot = lax.rem(step, 2)
    dst = out.at[:, pl.ds(pl.multiple_of(bit * 128 + rb(step) * RB, RB), RB), :]
    mine = theirs = st.at[slot]
    if split:
        mine = st.at[slot, :, :, pl.ds(pl.multiple_of(bit * 128, 128), 128)]
        theirs = st.at[slot, :, :, pl.ds(pl.multiple_of((1 - bit) * 128, 128), 128)]
    return slot, dst, mine, theirs


def pair_here(step, st, out, sems, split):
    slot, dst, mine, _ = pair_parts(step, st, out, split)
    return pltpu.make_async_copy(mine, dst, sems[0].at[slot])


def pair_there(step, st, out, sems, split):
    slot, dst, _, theirs = pair_parts(step, st, out, split)
    return remote(theirs, dst, sems[1].at[slot], sems[2].at[step], 0)


def ship(step, items):
    @pl.when(step >= 2)
    def _():
        for _, *it in items:
            pair_here(step - 2, *it).wait()
            pair_there(step - 2, *it).wait_send()
    for scr, *it in items:
        pack(scr, it[0].at[lax.rem(step, 2)])
        pair_here(step, *it).start()
        pair_there(step, *it).start()

    @pl.when(step == 7)
    def _():
        for _, *it in items:
            for k in (6, 7):
                pair_here(k, *it).wait()
                pair_there(k, *it).wait_send()
            for k in range(8):
                pair_there(k, *it).wait_recv()


def ship_scratch():
    return [pltpu.VMEM((2, C, RB, N), BF16), pltpu.SemaphoreType.DMA((2,)), pltpu.SemaphoreType.DMA((2,)), pltpu.SemaphoreType.DMA((8,))]


def pre_kernel(z_ref, m_ref, ln_ref, wt_ref, bp_ref, a_ref, zh_ref, zt_ref, mall_ref, af_ref, bf_ref,
               scr_a, scr_b, mbuf, zbuf, zloc, zsend, zrecv, msem, st_a, la, sa, ra, st_b, lb, sb, rb_):
    step = pl.program_id(0)
    xb = partner(1)[0]

    def z_here(q):
        return pltpu.make_async_copy(z_ref.at[pl.ds(q * RB, RB)], zbuf.at[pl.ds(q * RB, RB)], zloc.at[q])

    def z_there(q):
        return remote(z_ref.at[pl.ds(q * RB, RB)], zbuf.at[pl.ds(64 + q * RB, RB)], zsend.at[q], zrecv.at[q], 1)

    m_dst = mbuf.at[pl.ds(pl.multiple_of(xb * 64, 64), 64), :]

    def m_there():
        return remote(m_ref, m_dst, msem.at[1], msem.at[2], 1)

    @pl.when(step == 0)
    def _():
        for q in range(4):
            z_here(q).start()
        greet((0, 1))
        m_here = pltpu.make_async_copy(m_ref, m_dst, msem.at[0])
        m_here.start()
        m_there().start()
        for q in range(4):
            z_there(q).start()
        m_here.wait()
    for q in range(4):
        @pl.when(step == q)
        def _():
            z_here(q).wait()

        @pl.when(step == 4 + q)
        def _():
            if q == 0:
                m_there().wait()
            z_there(q).wait()

    def row(r, _):
        zt = load_t(zbuf, step * RB + r)
        zt_ref[r] = zt.astype(BF16)
        zn, _ = norm(zt)
        zh = (zn * ln_ref[0] + ln_ref[1]).astype(BF16)
        zh_ref[r] = zh
        gates(zh, mbuf[pl.ds(rb(step) * RB + r, 1), :], wt_ref, bp_ref, scr_a, scr_b, r)
        return 0
    lax.fori_loop(0, RB, row, 0, unroll=UN)
    ship(step, [(scr_a, st_a, af_ref, (la, sa, ra), False), (scr_b, st_b, bf_ref, (lb, sb, rb_), False)])
    a_ref[...] = st_a[lax.rem(step, 2)]

    @pl.when(step == 7)
    def _():
        mall_ref[...] = mbuf[...]


def mid_kernel(x_ref, zh_ref, zt_ref, m_ref, lnm_ref, wot_ref, bo_ref, wgt_ref, bg_ref, ln_ref, wt_ref, bp_ref,
               zm_ref, zh1_ref, ao_ref, bo1_ref, ac_ref, bf_ref, scr_x, scr_a, scr_b, st_a, la, sa, ra, st_b, lb, sb, rb_):
    step = pl.program_id(0)

    @pl.when(step == 0)
    def _():
        greet((0,))
    unpack(x_ref, scr_x)

    def row(r, _):
        xn, _ = norm(get_row(scr_x, r))
        xh = (xn * lnm_ref[0] + lnm_ref[1]).astype(BF16)
        u = dot(wot_ref[...], xh) + bo_ref[...]
        g = sig(dot(wgt_ref[...], zh_ref[r]) + bg_ref[...])
        zm = (zt_ref[r].astype(F32) + g * u).astype(BF16)
        zm_ref[r] = zm
        zn, _ = norm(zm.astype(F32))
        zh = (zn * ln_ref[0] + ln_ref[1]).astype(BF16)
        zh1_ref[r] = zh
        gates(zh, m_ref[pl.ds(r, 1), :], wt_ref, bp_ref, scr_a, scr_b, r)
        return 0
    lax.fori_loop(0, RB, row, 0, unroll=UN)
    ship(step, [(scr_a, st_a, ac_ref, (la, sa, ra), True), (scr_b, st_b, bf_ref, (lb, sb, rb_), False)])

    @pl.when(step < 4)
    def _():
        ao_ref[...] = st_a[lax.rem(step, 2)]
        bo1_ref[...] = st_b[lax.rem(step, 2)]


def post_row(x, zh, lnm_ref, wot_ref, wo_ref, bo_ref, wgt_ref, bg_ref, dz):
    xn, rstd = norm(x)
    xh = (xn * lnm_ref[0] + lnm_ref[1]).astype(BF16)
    u = dot(wot_ref[...], xh) + bo_ref[...]
    g = sig(dot(wgt_ref[...], zh) + bg_ref[...])
    d_pg = dz * u * (g * (1.0 - g))
    d_upd = dz * g
    d_bf = d_upd.astype(BF16)
    d_xh = dot(wo_ref[...], d_bf)
    dx = norm_bwd(d_xh, xn, rstd, lnm_ref[0])
    return xh, xn, u, g, d_pg, d_upd, d_bf, d_xh, dx


def post_grads(parts, dwo_ref, vec_ref):
    xh, xn, d_pg, d_upd, d_bf, d_xh = parts
    dwo_ref[...] += dot_t(xh, d_bf)
    vec_ref[0] += d_upd
    vec_ref[1] += d_xh * xn
    vec_ref[2] += d_xh
    vec_ref[3] += d_pg


def zero(*refs):
    for ref in refs:
        ref[...] = jnp.zeros_like(ref)


def post1_kernel(x_ref, zh_ref, zm_ref, dz_ref, dzo_ref, lnm_ref, wot_ref, wo_ref, bo_ref, wgt_ref, bg_ref,
                 zo_ref, dpg_ref, dzt_ref, dwo_ref, vec_ref, dxf_ref, scr_x, scr_d, st, lsem, ssem, rsem):
    step = pl.program_id(0)

    @pl.when(step == 0)
    def _():
        greet((0,))
        zero(dwo_ref, vec_ref)
    unpack(x_ref, scr_x)

    @pl.when(step >= 4)
    def _():
        def row(r, _):
            dz = load_t(dzo_ref, r)
            res = post_row(get_row(scr_x, r), zh_ref[r], lnm_ref, wot_ref, wo_ref, bo_ref, wgt_ref, bg_ref, dz)
            put_row(scr_d, r, res[-1])
            return 0
        lax.fori_loop(0, RB, row, 0, unroll=UN)

    @pl.when(step < 4)
    def _():
        def row(r, _):
            dz = load_t(dz_ref, r)
            dzt_ref[r] = dz.astype(BF16)
            xh, xn, u, g, d_pg, d_upd, d_bf, d_xh, dx = post_row(get_row(scr_x, r), zh_ref[r], lnm_ref, wot_ref, wo_ref, bo_ref, wgt_ref, bg_ref, dz)
            put_row(scr_d, r, dx)
            dpg_ref[r] = d_pg.astype(BF16)
            store_t(zo_ref, r, zm_ref[r].astype(F32) + g * u)
            post_grads((xh, xn, d_pg, d_upd, d_bf, d_xh), dwo_ref, vec_ref)
            return 0
        lax.fori_loop(0, RB, row, 0, unroll=UN)
    ship(step, [(scr_d, st, dxf_ref, (lsem, ssem, rsem), False)])


def pre_bwd_row(r, z, zh, m, d_pg, scr_a, scr_b, ln_ref, wt_ref, w_ref, bp_ref, dp_ref, dwp_ref, vec_ref, base):
    for q, scr in ((0, scr_a), (1, scr_b)):
        p = dot(wt_ref[q * 256:(q + 1) * 256, :], zh)
        s = sig(p[0:128] + bp_ref[2 * q])
        v = p[128:256] + bp_ref[2 * q + 1]
        d_s = get_row(scr, r) * m
        d_v = d_s * s
        d_g = d_v * v * (1.0 - s)
        dp_ref[q * 256:q * 256 + 128, :] = d_g.astype(BF16)
        dp_ref[q * 256 + 128:q * 256 + 256, :] = d_v.astype(BF16)
        vec_ref[base + 2 * q] += d_g
        vec_ref[base + 2 * q + 1] += d_v
    dp_ref[512:640, :] = d_pg
    dp = dp_ref[...]
    dwp_ref[...] += dot_t(dp, zh)
    d_zh = dot(w_ref[...], dp)
    zn, rstd = norm(z)
    vec_ref[base + 4] += d_zh * zn
    vec_ref[base + 5] += d_zh
    return norm_bwd(d_zh, zn, rstd, ln_ref[0])


def midb_kernel(da_ref, db_ref, zh1_ref, zm_ref, m_ref, dpg1_ref, dzt_ref, x0_ref, zh0_ref,
                ln_ref, wt_ref, w_ref, bp_ref, lnm_ref, wot_ref, wo_ref, bo_ref, wgt_ref, bg_ref,
                dzm_ref, dx_ref, dpg0_ref, dwp_ref, dwo_ref, vec_ref, vec2_ref, scr_a, scr_b, scr_x, scr_d, dp_ref):
    @pl.when(pl.program_id(0) == 0)
    def _():
        zero(dwp_ref, dwo_ref, vec_ref, vec2_ref)
    unpack(da_ref, scr_a)
    unpack(db_ref, scr_b)
    unpack(x0_ref, scr_x)

    def row(r, _):
        dz_norm = pre_bwd_row(r, zm_ref[r].astype(F32), zh1_ref[r], m_ref[pl.ds(r, 1), :], dpg1_ref[r], scr_a, scr_b,
                              ln_ref, wt_ref, w_ref, bp_ref, dp_ref, dwp_ref, vec_ref, 0)
        dzm = (dzt_ref[r].astype(F32) + dz_norm).astype(BF16)
        dzm_ref[r] = dzm
        xh, xn, u, g, d_pg, d_upd, d_bf, d_xh, dx = post_row(get_row(scr_x, r), zh0_ref[r], lnm_ref, wot_ref, wo_ref, bo_ref, wgt_ref, bg_ref, dzm.astype(F32))
        put_row(scr_d, r, dx)
        dpg0_ref[r] = d_pg.astype(BF16)
        post_grads((xh, xn, d_pg, d_upd, d_bf, d_xh), dwo_ref, vec2_ref)
        return 0
    lax.fori_loop(0, RB, row, 0, unroll=UN)
    pack(scr_d, dx_ref)


def last_kernel(da_ref, db_ref, zh_ref, zt_ref, m_ref, dpg_ref, dzm_ref, ln_ref, wt_ref, w_ref, bp_ref,
                dz_ref, dwp_ref, vec_ref, scr_a, scr_b, dp_ref):
    @pl.when(pl.program_id(0) == 0)
    def _():
        zero(dwp_ref, vec_ref)
    unpack(da_ref, scr_a)
    unpack(db_ref, scr_b)

    def row(r, _):
        dz_norm = pre_bwd_row(r, zt_ref[r].astype(F32), zh_ref[r], m_ref[pl.ds(r, 1), :], dpg_ref[r], scr_a, scr_b,
                              ln_ref, wt_ref, w_ref, bp_ref, dp_ref, dwp_ref, vec_ref, 0)
        store_t(dz_ref, r, dzm_ref[r].astype(F32) + dz_norm)
        return 0
    lax.fori_loop(0, RB, row, 0, unroll=UN)


def sds(shape, dtype):
    return jax.ShapeDtypeStruct(shape, dtype)


def full(shape):
    nd = len(shape)
    return pl.BlockSpec(shape, lambda *_: (0,) * nd)


def rows_spec(shape, fn):
    return pl.BlockSpec((RB,) + shape, lambda i: (fn(i),) + (0,) * len(shape))


def cm_spec(fn):
    return pl.BlockSpec((C, RB, N), lambda i: (0, fn(i), 0))


def scr():
    return pltpu.VMEM((2, C * SP, 128), F32)


ANY = pl.BlockSpec(memory_space=pl.ANY)


def call(kernel, grid, in_specs, out_specs, out_shape, scratch, name, cid=None):
    return pl.pallas_call(
        kernel, name=name, out_shape=out_shape, grid=(grid,), in_specs=in_specs, out_specs=out_specs, scratch_shapes=scratch,
        compiler_params=pltpu.CompilerParams(dimension_semantics=("arbitrary",), vmem_limit_bytes=60 << 20, collective_id=cid, has_side_effects=cid is not None))


def reduce_kernel(dwp0_ref, dwo0_ref, pre0_ref, post0_ref, dwp1_ref, dwo1_ref, pre1_ref, post1_ref, out_ref, acc, got0, got1, got2, got3, send, recv):
    greet((0, 1, 2, 3))
    parts = ((dwp0_ref, dwo0_ref, pre0_ref, post0_ref), (dwp1_ref, dwo1_ref, pre1_ref, post1_ref))
    for k, (dwp, dwo, vpre, vpost) in enumerate(parts):
        acc[784 * k:784 * k + 640, :] = dwp[...]
        acc[784 * k + 640:784 * k + 768, :] = dwo[...]
        rows = [jnp.sum(jnp.transpose(v[q]), axis=0, keepdims=True) for v, n in ((vpre, 6), (vpost, 4)) for q in range(n)]
        acc[784 * k + 768:784 * k + 784, :] = jnp.concatenate(rows + [jnp.zeros((6, C), F32)], axis=0)
    acc[1568:GROWS, :] = jnp.zeros((GROWS - 1568, C), F32)
    got = (got0, got1, got2, got3)
    spans = [[r0, n] for r0, n, _ in CHUNKS]
    for st in range(4):
        copies = []
        base = 0
        for ch, (_, _, order) in enumerate(CHUNKS):
            lo, n = spans[ch]
            half = n // 2
            bit = partner(order[st])[0]
            give = pl.multiple_of(lo + (1 - bit) * half, 8)
            keep = pl.multiple_of(lo + bit * half, 8)
            land = got[st].at[pl.ds(base, half), :]
            cp = remote(acc.at[pl.ds(give, half), :], land, send.at[st, ch], recv.at[st, ch], order[st])
            cp.start()
            copies.append((cp, keep, half, base))
            spans[ch] = [keep, half]
            base += half
        for cp, keep, half, base in copies:
            cp.wait()
            acc[pl.ds(keep, half), :] += got[st][base:base + half, :]
    for lo, n in spans:
        out_ref[pl.ds(lo, n), :] = acc[pl.ds(lo, n), :]
    for st in (3, 2, 1, 0):
        copies = []
        for ch, (_, _, order) in enumerate(CHUNKS):
            lo, n = spans[ch]
            bit = partner(order[st])[0]
            seg = out_ref.at[pl.ds(pl.multiple_of(lo, 8), n), :]
            cp = remote(seg, seg, send.at[4 + st, ch], recv.at[4 + st, ch], order[st])
            cp.start()
            copies.append(cp)
            spans[ch] = [lo - bit * n, 2 * n]
        for cp in copies:
            cp.wait()


def reduce_all(*g):
    vm = pl.BlockSpec(memory_space=pltpu.VMEM)
    return pl.pallas_call(
        reduce_kernel, name="reduce", out_shape=sds((GROWS, C), F32), in_specs=[vm] * 8, out_specs=vm,
        scratch_shapes=[pltpu.VMEM((GROWS, C), F32)] + [pltpu.VMEM((GROWS >> (k + 1), C), F32) for k in range(4)]
        + [pltpu.SemaphoreType.DMA((8, 3)), pltpu.SemaphoreType.DMA((8, 3))],
        compiler_params=pltpu.CompilerParams(collective_id=0, has_side_effects=True))(*g)


def solution(mesh):
    def local_step(z_pair, pair_mask, dz_out, ln_in, w_proj, b_proj, ln_mid, w_out, b_out):
        mask = pair_mask[0].reshape(64, 2, 2, 64).transpose(0, 2, 1, 3).reshape(64, N).astype(F32)

        def wide(v):
            return jnp.broadcast_to(v.astype(F32)[..., None], v.shape + (N,))

        lni = wide(ln_in)
        lnm = wide(ln_mid)
        bp = wide(b_proj.reshape(2, 5, C))
        bo = wide(b_out)
        wt = jnp.swapaxes(w_proj, 1, 2)
        wot = jnp.swapaxes(w_out, 1, 2)

        same = lambda i: i
        cm_all = sds((C, 128, N), BF16)
        cm_full = sds((C, N, N), BF16)
        cm_own = sds((C, 64, N), BF16)
        rt_all = sds((128, C, N), BF16)
        rt_own = sds((64, C, N), BF16)
        vm = pl.BlockSpec(memory_space=pltpu.VMEM)

        a0, zh0, zt0, mask_all, a0f, b0f = call(
            pre_kernel, 8, [ANY, vm, full((2, C, N)), full((512, C)), full((5, C, N))],
            [cm_spec(rb), rows_spec((C, N), rb), rows_spec((C, N), rb), vm, ANY, ANY],
            [cm_all, rt_all, rt_all, sds((128, N), F32), cm_full, cm_full],
            [scr(), scr(), pltpu.VMEM((128, N), F32), pltpu.VMEM((128, N, C), BF16)] + [pltpu.SemaphoreType.DMA((4,))] * 3 + [pltpu.SemaphoreType.DMA((3,))] + ship_scratch() * 2,
            "pre", 1)(z_pair[0], mask, lni[0], wt[0, :512], bp[0])
        dz_own, a0 = lax.optimization_barrier((dz_out[0], a0))
        dz_oth = lax.ppermute(dz_own, "dap", SWAP_X)
        x0 = jnp.einsum("cik,cjk->cij", a0, b0f, preferred_element_type=F32)

        sm = [full((2, C, N)), full((C, C)), full((C, N)), full((C, C)), full((C, N))]
        zm, zh1, a1o, b1o, a1c, b1f = call(
            mid_kernel, 8,
            [cm_spec(rb), rows_spec((C, N), rb), rows_spec((C, N), rb), rows_spec((N,), rb)] + sm + [full((2, C, N)), full((512, C)), full((5, C, N))],
            [rows_spec((C, N), rb), rows_spec((C, N), rb), cm_spec(first4), cm_spec(first4), ANY, ANY],
            [rt_all, rt_all, cm_own, cm_own, sds((C, N, 128), BF16), cm_full],
            [scr(), scr(), scr()] + ship_scratch()[:0] + [pltpu.VMEM((2, C, RB, N), BF16)] + ship_scratch()[1:] + ship_scratch(),
            "mid", 2)(x0, zh0, zt0, mask_all, lnm[0], wot[0], bo[0], wt[0, 512:], bp[0, 4], lni[1], wt[1, :512], bp[1])
        x1 = jnp.einsum("cki,ckj->cij", a1c, b1f, preferred_element_type=F32)

        late = lambda i: lax.max(i - 4, 0)
        smb = [full((2, C, N)), full((C, C)), full((C, C)), full((C, N)), full((C, C)), full((C, N))]
        zo, dpg1, dzt, dwo1, vec1, dx1f = call(
            post1_kernel, 8,
            [cm_spec(rb), rows_spec((C, N), rb), rows_spec((C, N), rb), rows_spec((N, C), first4), rows_spec((N, C), late)] + smb,
            [rows_spec((N, C), first4), rows_spec((C, N), first4), rows_spec((C, N), first4), full((C, C)), full((4, C, N)), ANY],
            [sds((64, N, C), BF16), rt_own, rt_own, sds((C, C), F32), sds((4, C, N), F32), cm_full],
            [scr(), scr()] + ship_scratch(), "post1", 3)(
            x1, zh1, zm, dz_own, dz_oth, lnm[1], wot[1], w_out[1], bo[1], wt[1, 512:], bp[1, 4])
        da1 = jnp.einsum("ckj,cij->cki", b1o, dx1f, preferred_element_type=F32).astype(BF16)
        db1 = jnp.einsum("cki,cij->ckj", a1o, dx1f, preferred_element_type=F32).astype(BF16)

        own = lambda i: i + 4 * partner(1)[0]
        wp = [full((2, C, N)), full((640, C)), full((C, 640)), full((5, C, N))]
        dzm, dx0, dpg0, dwp1, dwo0, vec2, vec3 = call(
            midb_kernel, 4,
            [cm_spec(same), cm_spec(same), rows_spec((C, N), own), rows_spec((C, N), own), rows_spec((N,), own),
             rows_spec((C, N), same), rows_spec((C, N), same), cm_spec(own), rows_spec((C, N), own)] + wp + smb,
            [rows_spec((C, N), same), cm_spec(same), rows_spec((C, N), same), full((640, C)), full((C, C)), full((6, C, N)), full((4, C, N))],
            [rt_own, sds((C, 64, N), BF16), rt_own, sds((640, C), F32), sds((C, C), F32), sds((6, C, N), F32), sds((4, C, N), F32)],
            [scr(), scr(), scr(), scr(), pltpu.VMEM((640, N), BF16)], "midb")(
            da1, db1, zh1, zm, mask_all, dpg1, dzt, x0, zh0, lni[1], wt[1], w_proj[1], bp[1],
            lnm[0], wot[0], w_out[0], bo[0], wt[0, 512:], bp[0, 4])
        dx0c = lax.all_to_all(dx0, "dap", 2, 1, axis_index_groups=QUAD, tiled=True)
        da0 = jnp.einsum("cij,cjk->cik", dx0, b0f, preferred_element_type=F32).astype(BF16)
        db0 = jnp.einsum("cij,cik->cjk", dx0c, a0f, preferred_element_type=F32).astype(BF16)

        dzp, dwp0, vec4 = call(
            last_kernel, 4,
            [cm_spec(same), cm_spec(same), rows_spec((C, N), own), rows_spec((C, N), own), rows_spec((N,), own),
             rows_spec((C, N), same), rows_spec((C, N), same)] + wp,
            [rows_spec((N, C), same), full((640, C)), full((6, C, N))],
            [sds((64, N, C), BF16), sds((640, C), F32), sds((6, C, N), F32)],
            [scr(), scr(), pltpu.VMEM((640, N), BF16)], "last")(
            da0, db0, zh0, zt0, mask_all, dpg0, dzm, lni[0], wt[0], w_proj[0], bp[0])

        g = reduce_all(dwp0, dwo0, vec4, vec3, dwp1, dwo1, vec2, vec1)[:1568].reshape(2, 784, C)
        d_b = jnp.concatenate([g[:, 768:772].reshape(2, 512), g[:, 777]], axis=1)
        return (zo[None], dzp[None], g[:, 772:774], jnp.swapaxes(g[:, :640], 1, 2), d_b, g[:, 775:777], g[:, 640:768], g[:, 774])

    row_spec = P("dp", "dap")
    return jax.shard_map(local_step, mesh=mesh, in_specs=(row_spec, row_spec, row_spec, P(), P(), P(), P(), P(), P()), out_specs=(row_spec, row_spec, P(), P(), P(), P(), P(), P()), check_vma=False)
```

```python
import functools
import jax
import jax.numpy as jnp
from jax import lax
from jax.experimental import pallas as pl
from jax.experimental.pallas import tpu as pltpu
from jax.sharding import PartitionSpec as P

LN_EPS = 1e-5
RB = 16
SP = 17
UN = 8
GR = 4
F32 = jnp.float32
BF16 = jnp.bfloat16
C = 128
N = 256
SWAP_X = [(0, 2), (2, 0), (1, 3), (3, 1)]


def dot(a, b):
    return lax.dot_general(a, b, (((1,), (0,)), ((), ())), preferred_element_type=F32)


def dot_t(a, b):
    return dot(a, jnp.transpose(b))


def sig(v):
    return 0.5 * jnp.tanh(0.5 * v) + 0.5


def norm(v):
    mu = jnp.mean(v, axis=0, keepdims=True)
    vc = v - mu
    rstd = lax.rsqrt(jnp.mean(vc * vc, axis=0, keepdims=True) + LN_EPS)
    return vc * rstd, rstd


def norm_bwd(d_hat, vn, rstd, gain):
    dn = d_hat * gain
    m1 = jnp.mean(dn, axis=0, keepdims=True)
    m2 = jnp.mean(dn * vn, axis=0, keepdims=True)
    return rstd * (dn - m1 - vn * m2)


def perm_cols(t):
    return jnp.concatenate([t[0:64], t[128:192], t[64:128], t[192:256]], axis=0)


def load_t(ref, r):
    return jnp.transpose(perm_cols(ref[r])).astype(F32)


def store_t(ref, r, val):
    ref[r] = perm_cols(jnp.transpose(val))


def by_chip(v):
    v0, v1 = v[:, :128], v[:, 128:]
    low = lax.broadcasted_iota(jnp.int32, (C, 128), 1) < 64
    return jnp.concatenate([jnp.where(low, v0, pltpu.roll(v1, 64, 1)), jnp.where(low, pltpu.roll(v0, 64, 1), v1)], axis=1)


def put_row(scr, r, val):
    for h in range(2):
        scr[h, pl.ds(r, C, stride=SP), :] = val[:, h * 128:(h + 1) * 128]


def get_row(scr, r):
    return jnp.concatenate([scr[h, pl.ds(r, C, stride=SP), :] for h in range(2)], axis=1)


def pack(scr, out_ref):
    def body(i, _):
        c0 = i * 8
        for k in range(8):
            for h in range(2):
                out_ref[c0 + k, :, h * 128:(h + 1) * 128] = scr[h, pl.ds((c0 + k) * SP, RB), :].astype(out_ref.dtype)
        return 0
    lax.fori_loop(0, C // 8, body, 0)


def unpack(in_ref, scr):
    def body(i, _):
        c0 = i * 8
        for k in range(8):
            for h in range(2):
                scr[h, pl.ds((c0 + k) * SP, RB), :] = in_ref[c0 + k, :, h * 128:(h + 1) * 128].astype(F32)
        return 0
    lax.fori_loop(0, C // 8, body, 0)


def gates(zh, m, wt, bp, scr_a, scr_b, g_ref, r):
    p = dot(wt[...], zh)
    put_row(scr_a, r, sig(p[0:128] + bp[0]) * (p[128:256] + bp[1]) * m)
    put_row(scr_b, r, sig(p[256:384] + bp[2]) * (p[384:512] + bp[3]) * m)
    g_ref[r] = sig(p[512:640] + bp[4])


def groups(body):
    lax.fori_loop(0, RB // GR, body, 0)


def halves(v):
    return v[:, :128] + v[:, 128:]


CHUNKS = ((0, 640, (0, 1, 2, 3)), (640, 512, (0, 2, 3, 1)), (1152, 512, (0, 3, 1, 2)))
GROWS = 1664


def coords():
    return lax.axis_index("dp"), lax.axis_index("dap")


def partner(k):
    dp, dap = coords()
    if k < 2:
        bit = lax.rem(dap // (1 << k), 2)
        return bit, (dp, dap + (1 << k) * (1 - 2 * bit))
    bit = lax.rem(dp // (1 << (k - 2)), 2)
    return bit, (dp + (1 << (k - 2)) * (1 - 2 * bit), dap)


def greet(keys):
    barrier = pltpu.get_barrier_semaphore()
    for k in keys:
        pl.semaphore_signal(barrier, inc=1, device_id=partner(k)[1], device_id_type=pl.DeviceIdType.MESH)
    pl.semaphore_wait(barrier, len(keys))


def remote(src, dst, send, recv, k):
    return pltpu.make_async_remote_copy(src_ref=src, dst_ref=dst, send_sem=send, recv_sem=recv, device_id=partner(k)[1], device_id_type=pl.DeviceIdType.MESH)


def rb(i):
    return lax.rem(i + 4 * partner(1)[0], 8)


def first4(i):
    return lax.min(i, 3)


def pair_parts(step, st, out, split):
    bit = partner(0)[0]
    slot = lax.rem(step, 2)
    dst = out.at[:, pl.ds(pl.multiple_of(bit * 128 + rb(step) * RB, RB), RB), :]
    mine = theirs = st.at[slot]
    if split:
        mine = st.at[slot, :, :, pl.ds(pl.multiple_of(bit * 128, 128), 128)]
        theirs = st.at[slot, :, :, pl.ds(pl.multiple_of((1 - bit) * 128, 128), 128)]
    return slot, dst, mine, theirs


def pair_here(step, st, out, sems, split):
    slot, dst, mine, _ = pair_parts(step, st, out, split)
    return pltpu.make_async_copy(mine, dst, sems[0].at[slot])


def pair_there(step, st, out, sems, split):
    slot, dst, _, theirs = pair_parts(step, st, out, split)
    return remote(theirs, dst, sems[1].at[slot], sems[2].at[step], 0)


def ship(step, items):
    @pl.when(step >= 2)
    def _():
        for _, *it in items:
            pair_here(step - 2, *it).wait()
            pair_there(step - 2, *it).wait_send()
    for scr, *it in items:
        pack(scr, it[0].at[lax.rem(step, 2)])
        pair_here(step, *it).start()
        pair_there(step, *it).start()

    @pl.when(step == 7)
    def _():
        for _, *it in items:
            for k in (6, 7):
                pair_here(k, *it).wait()
                pair_there(k, *it).wait_send()
            for k in range(8):
                pair_there(k, *it).wait_recv()


def ship_scratch():
    return [pltpu.VMEM((2, C, RB, N), BF16), pltpu.SemaphoreType.DMA((2,)), pltpu.SemaphoreType.DMA((2,)), pltpu.SemaphoreType.DMA((8,))]


def pre_kernel(z_ref, m_ref, ln_ref, wt_ref, bp_ref, a_ref, zh_ref, zt_ref, g_ref, mall_ref, af_ref, bf_ref,
               scr_a, scr_b, mbuf, zbuf, zloc, zsend, zrecv, msem, st_a, la, sa, ra, st_b, lb, sb, rb_):
    step = pl.program_id(0)
    xb = partner(1)[0]

    def z_here(q):
        return pltpu.make_async_copy(z_ref.at[pl.ds(q * RB, RB)], zbuf.at[pl.ds(q * RB, RB)], zloc.at[q])

    def z_there(q):
        return remote(z_ref.at[pl.ds(q * RB, RB)], zbuf.at[pl.ds(64 + q * RB, RB)], zsend.at[q], zrecv.at[q], 1)

    m_dst = mbuf.at[pl.ds(pl.multiple_of(xb * 64, 64), 64), :]

    def m_there():
        return remote(m_ref, m_dst, msem.at[1], msem.at[2], 1)

    @pl.when(step == 0)
    def _():
        for q in range(4):
            z_here(q).start()
        greet((0, 1))
        m_here = pltpu.make_async_copy(m_ref, m_dst, msem.at[0])
        m_here.start()
        m_there().start()
        for q in range(4):
            z_there(q).start()
        m_here.wait()
    for q in range(4):
        @pl.when(step == q)
        def _():
            z_here(q).wait()

        @pl.when(step == 4 + q)
        def _():
            if q == 0:
                m_there().wait()
            z_there(q).wait()

    def row(r, _):
        zt = load_t(zbuf, step * RB + r)
        zt_ref[r] = zt.astype(BF16)
        zn, _ = norm(zt)
        zh = (zn * ln_ref[0] + ln_ref[1]).astype(BF16)
        zh_ref[r] = zh
        gates(zh, mbuf[pl.ds(rb(step) * RB + r, 1), :], wt_ref, bp_ref, scr_a, scr_b, g_ref, r)
        return 0
    lax.fori_loop(0, RB, row, 0, unroll=UN)
    ship(step, [(scr_a, st_a, af_ref, (la, sa, ra), False), (scr_b, st_b, bf_ref, (lb, sb, rb_), False)])
    a_ref[...] = st_a[lax.rem(step, 2)]

    @pl.when(step == 7)
    def _():
        mall_ref[...] = mbuf[...]


def mid_kernel(x_ref, g_ref, zt_ref, m_ref, lnm_ref, wot_ref, bo_ref, ln_ref, wt_ref, bp_ref,
               zm_ref, zh1_ref, g1_ref, ao_ref, bo1_ref, ac_ref, bf_ref, scr_x, scr_a, scr_b, st_a, la, sa, ra, st_b, lb, sb, rb_):
    step = pl.program_id(0)

    @pl.when(step == 0)
    def _():
        greet((0,))
    unpack(x_ref, scr_x)

    def row(r, _):
        xn, _ = norm(get_row(scr_x, r))
        xh = (xn * lnm_ref[0] + lnm_ref[1]).astype(BF16)
        u = dot(wot_ref[...], xh) + bo_ref[...]
        zm = (zt_ref[r].astype(F32) + g_ref[r] * u).astype(BF16)
        zm_ref[r] = zm
        zn, _ = norm(zm.astype(F32))
        zh = (zn * ln_ref[0] + ln_ref[1]).astype(BF16)
        zh1_ref[r] = zh
        gates(zh, m_ref[pl.ds(r, 1), :], wt_ref, bp_ref, scr_a, scr_b, g1_ref, r)
        return 0
    lax.fori_loop(0, RB, row, 0, unroll=UN)
    ship(step, [(scr_a, st_a, ac_ref, (la, sa, ra), True), (scr_b, st_b, bf_ref, (lb, sb, rb_), False)])

    @pl.when(step < 4)
    def _():
        ao_ref[...] = st_a[lax.rem(step, 2)]
        bo1_ref[...] = st_b[lax.rem(step, 2)]


def post_row(x, g, lnm_ref, wot_ref, wo_ref, bo_ref, dz):
    xn, rstd = norm(x)
    xh = (xn * lnm_ref[0] + lnm_ref[1]).astype(BF16)
    u = dot(wot_ref[...], xh) + bo_ref[...]
    d_pg = dz * u * (g * (1.0 - g))
    d_upd = dz * g
    d_bf = d_upd.astype(BF16)
    d_xh = dot(wo_ref[...], d_bf)
    dx = norm_bwd(d_xh, xn, rstd, lnm_ref[0])
    return xh, xn, u, d_pg, d_upd, d_bf, d_xh, dx


def post_vecs(vec_ref, d_upd, d_xh, xn, d_pg):
    for q, v in enumerate((d_upd, d_xh * xn, d_xh, d_pg)):
        vec_ref[q] += halves(v)


def add_outer(acc_ref, left, right):
    acc_ref[...] += dot(jnp.concatenate(left, axis=1), jnp.transpose(jnp.concatenate(right, axis=1)))


def zero(*refs):
    for ref in refs:
        ref[...] = jnp.zeros_like(ref)


def post1_kernel(x_ref, g_ref, zm_ref, dz_ref, dzo_ref, lnm_ref, wot_ref, wo_ref, bo_ref,
                 zo_ref, dpg_ref, dzt_ref, dwo_ref, vec_ref, dxf_ref, scr_x, scr_d, st, lsem, ssem, rsem):
    step = pl.program_id(0)

    @pl.when(step == 0)
    def _():
        greet((0,))
        zero(dwo_ref, vec_ref)
    unpack(x_ref, scr_x)

    @pl.when(step >= 4)
    def _():
        def row(r, _):
            dz = load_t(dzo_ref, r)
            res = post_row(get_row(scr_x, r), g_ref[r], lnm_ref, wot_ref, wo_ref, bo_ref, dz)
            put_row(scr_d, r, res[-1])
            return 0
        lax.fori_loop(0, RB, row, 0, unroll=GR)

    @pl.when(step < 4)
    def _():
        def group(i, _):
            left, right = [], []
            for k in range(GR):
                r = i * GR + k
                dz = load_t(dz_ref, r)
                dzt_ref[r] = dz.astype(BF16)
                g = g_ref[r]
                xh, xn, u, d_pg, d_upd, d_bf, d_xh, dx = post_row(get_row(scr_x, r), g, lnm_ref, wot_ref, wo_ref, bo_ref, dz)
                put_row(scr_d, r, dx)
                dpg_ref[r] = d_pg.astype(BF16)
                zo_ref[r] = (zm_ref[r].astype(F32) + g * u).astype(BF16)
                post_vecs(vec_ref, d_upd, d_xh, xn, d_pg)
                left.append(xh)
                right.append(d_bf)
            add_outer(dwo_ref, left, right)
            return 0
        groups(group)
    ship(step, [(scr_d, st, dxf_ref, (lsem, ssem, rsem), False)])


def pre_bwd_row(r, k, z, zh, m, d_pg, scr_a, scr_b, ln_ref, wt_ref, w_ref, bp_ref, dp_ref, vec_ref):
    p = dot(wt_ref[0:512, :], zh)
    cols = slice(k * N, k * N + N)
    for q, scr in ((0, scr_a), (1, scr_b)):
        s = sig(p[q * 256:q * 256 + 128] + bp_ref[2 * q])
        v = p[q * 256 + 128:q * 256 + 256] + bp_ref[2 * q + 1]
        d_s = get_row(scr, r) * m
        d_v = d_s * s
        d_g = d_v * v * (1.0 - s)
        dp_ref[q * 256:q * 256 + 128, cols] = d_g.astype(BF16)
        dp_ref[q * 256 + 128:q * 256 + 256, cols] = d_v.astype(BF16)
        vec_ref[2 * q] += halves(d_g)
        vec_ref[2 * q + 1] += halves(d_v)
    dp_ref[512:640, cols] = d_pg
    d_zh = dot(w_ref[...], dp_ref[:, cols])
    zn, rstd = norm(z)
    vec_ref[4] += halves(d_zh * zn)
    vec_ref[5] += halves(d_zh)
    return norm_bwd(d_zh, zn, rstd, ln_ref[0])


def midb_kernel(da_ref, db_ref, zh1_ref, zm_ref, m_ref, dpg1_ref, dzt_ref, x0_ref, g0_ref,
                ln_ref, wt_ref, w_ref, bp_ref, lnm_ref, wot_ref, wo_ref, bo_ref,
                dzm_ref, dx_ref, dpg0_ref, dwp_ref, dwo_ref, vec_ref, vec2_ref, dxk_ref, scr_a, scr_b, scr_x, scr_d, dp_ref,
                scr_e, st, lsem, csend, crecv, xsend, xrecv, rsend, rrecv):
    step = pl.program_id(0)
    cbit = partner(0)[0]
    xbit = partner(1)[0]

    def block(core, chip, k):
        return dxk_ref.at[:, pl.ds(pl.multiple_of(core * 128 + chip * 64 + k * RB, RB), RB), :]

    def part(k, chip):
        return st.at[lax.rem(k, 2), :, :, pl.ds(pl.multiple_of(chip * 128, 128), 128)]

    def here(k):
        return pltpu.make_async_copy(part(k, xbit), block(cbit, xbit, k), lsem.at[lax.rem(k, 2)])

    def to_core(k):
        return remote(part(k, xbit), block(cbit, xbit, k), csend.at[lax.rem(k, 2)], crecv.at[k], 0)

    def to_chip(k):
        return remote(part(k, 1 - xbit), block(cbit, xbit, k), xsend.at[lax.rem(k, 2)], xrecv.at[k], 1)

    def relay(k):
        blk = block(cbit, 1 - xbit, k)
        return remote(blk, blk, rsend.at[k], rrecv.at[k], 0)

    def settle(k):
        here(k).wait()
        to_core(k).wait_send()
        to_chip(k).wait_send()

    @pl.when(step == 0)
    def _():
        greet((0, 1))
        zero(dwp_ref, dwo_ref, vec_ref, vec2_ref)
    unpack(da_ref, scr_a)
    unpack(db_ref, scr_b)
    unpack(x0_ref, scr_x)

    def group(i, _):
        left, right, zhs = [], [], []
        for k in range(GR):
            r = i * GR + k
            zh = zh1_ref[r]
            zhs.append(zh)
            dz_norm = pre_bwd_row(r, k, zm_ref[r].astype(F32), zh, m_ref[pl.ds(r, 1), :], dpg1_ref[r], scr_a, scr_b,
                                  ln_ref, wt_ref, w_ref, bp_ref, dp_ref, vec_ref)
            dzm = (dzt_ref[r].astype(F32) + dz_norm).astype(BF16)
            dzm_ref[r] = dzm
            xh, xn, u, d_pg, d_upd, d_bf, d_xh, dx = post_row(get_row(scr_x, r), g0_ref[r], lnm_ref, wot_ref, wo_ref, bo_ref, dzm.astype(F32))
            put_row(scr_d, r, dx)
            put_row(scr_e, r, by_chip(dx))
            dpg0_ref[r] = d_pg.astype(BF16)
            post_vecs(vec2_ref, d_upd, d_xh, xn, d_pg)
            left.append(xh)
            right.append(d_bf)
        add_outer(dwo_ref, left, right)
        add_outer(dwp_ref, [dp_ref[...]], zhs)
        return 0
    groups(group)

    @pl.when(step >= 2)
    def _():
        settle(step - 2)
    pack(scr_e, st.at[lax.rem(step, 2)])
    to_chip(step).start()
    to_core(step).start()
    here(step).start()
    pack(scr_d, dx_ref)

    @pl.when(step >= 2)
    def _():
        to_chip(step - 2).wait_recv()
        relay(step - 2).start()

    @pl.when(step == 3)
    def _():
        for k in (2, 3):
            to_chip(k).wait_recv()
            relay(k).start()
            settle(k)
        for k in range(4):
            to_core(k).wait_recv()
            relay(k).wait()


def last_kernel(da_ref, db_ref, zh_ref, zt_ref, m_ref, dpg_ref, dzm_ref, zo_ref, ln_ref, wt_ref, w_ref, bp_ref,
                dz_ref, zout_ref, dwp_ref, vec_ref, scr_a, scr_b, dp_ref):
    @pl.when(pl.program_id(0) == 0)
    def _():
        zero(dwp_ref, vec_ref)
    unpack(da_ref, scr_a)
    unpack(db_ref, scr_b)

    def group(i, _):
        zhs = []
        for k in range(GR):
            r = i * GR + k
            zh = zh_ref[r]
            zhs.append(zh)
            dz_norm = pre_bwd_row(r, k, zt_ref[r].astype(F32), zh, m_ref[pl.ds(r, 1), :], dpg_ref[r], scr_a, scr_b,
                                  ln_ref, wt_ref, w_ref, bp_ref, dp_ref, vec_ref)
            store_t(dz_ref, r, (dzm_ref[r].astype(F32) + dz_norm).astype(BF16))
            store_t(zout_ref, r, zo_ref[r])
        add_outer(dwp_ref, [dp_ref[...]], zhs)
        return 0
    groups(group)


def sds(shape, dtype):
    return jax.ShapeDtypeStruct(shape, dtype)


def full(shape):
    nd = len(shape)
    return pl.BlockSpec(shape, lambda *_: (0,) * nd)


def rows_spec(shape, fn):
    return pl.BlockSpec((RB,) + shape, lambda i: (fn(i),) + (0,) * len(shape))


def cm_spec(fn):
    return pl.BlockSpec((C, RB, N), lambda i: (0, fn(i), 0))


def scr():
    return pltpu.VMEM((2, C * SP, 128), F32)


ANY = pl.BlockSpec(memory_space=pl.ANY)


def call(kernel, grid, in_specs, out_specs, out_shape, scratch, name, cid=None):
    return pl.pallas_call(
        kernel, name=name, out_shape=out_shape, grid=(grid,), in_specs=in_specs, out_specs=out_specs, scratch_shapes=scratch,
        compiler_params=pltpu.CompilerParams(dimension_semantics=("arbitrary",), vmem_limit_bytes=60 << 20, collective_id=cid, has_side_effects=cid is not None))


def reduce_kernel(dwp0_ref, dwo0_ref, pre0_ref, post0_ref, dwp1_ref, dwo1_ref, pre1_ref, post1_ref, out_ref, acc, got0, got1, got2, got3, send, recv):
    greet((0, 1, 2, 3))
    parts = ((dwp0_ref, dwo0_ref, pre0_ref, post0_ref), (dwp1_ref, dwo1_ref, pre1_ref, post1_ref))
    for k, (dwp, dwo, vpre, vpost) in enumerate(parts):
        acc[784 * k:784 * k + 640, :] = dwp[...]
        acc[784 * k + 640:784 * k + 768, :] = dwo[...]
        rows = [jnp.sum(jnp.transpose(v[q]), axis=0, keepdims=True) for v, n in ((vpre, 6), (vpost, 4)) for q in range(n)]
        acc[784 * k + 768:784 * k + 784, :] = jnp.concatenate(rows + [jnp.zeros((6, C), F32)], axis=0)
    acc[1568:GROWS, :] = jnp.zeros((GROWS - 1568, C), F32)
    got = (got0, got1, got2, got3)
    spans = [[r0, n] for r0, n, _ in CHUNKS]
    for st in range(4):
        copies = []
        base = 0
        for ch, (_, _, order) in enumerate(CHUNKS):
            lo, n = spans[ch]
            half = n // 2
            bit = partner(order[st])[0]
            give = pl.multiple_of(lo + (1 - bit) * half, 8)
            keep = pl.multiple_of(lo + bit * half, 8)
            land = got[st].at[pl.ds(base, half), :]
            cp = remote(acc.at[pl.ds(give, half), :], land, send.at[st, ch], recv.at[st, ch], order[st])
            cp.start()
            copies.append((cp, keep, half, base))
            spans[ch] = [keep, half]
            base += half
        for cp, keep, half, base in copies:
            cp.wait()
            acc[pl.ds(keep, half), :] += got[st][base:base + half, :]
    for lo, n in spans:
        out_ref[pl.ds(lo, n), :] = acc[pl.ds(lo, n), :]
    for st in (3, 2, 1, 0):
        copies = []
        for ch, (_, _, order) in enumerate(CHUNKS):
            lo, n = spans[ch]
            bit = partner(order[st])[0]
            seg = out_ref.at[pl.ds(pl.multiple_of(lo, 8), n), :]
            cp = remote(seg, seg, send.at[4 + st, ch], recv.at[4 + st, ch], order[st])
            cp.start()
            copies.append(cp)
            spans[ch] = [lo - bit * n, 2 * n]
        for cp in copies:
            cp.wait()


def reduce_all(*g):
    vm = pl.BlockSpec(memory_space=pltpu.VMEM)
    return pl.pallas_call(
        reduce_kernel, name="reduce", out_shape=sds((GROWS, C), F32), in_specs=[vm] * 8, out_specs=vm,
        scratch_shapes=[pltpu.VMEM((GROWS, C), F32)] + [pltpu.VMEM((GROWS >> (k + 1), C), F32) for k in range(4)]
        + [pltpu.SemaphoreType.DMA((8, 3)), pltpu.SemaphoreType.DMA((8, 3))],
        compiler_params=pltpu.CompilerParams(collective_id=0, has_side_effects=True))(*g)


def solution(mesh):
    def local_step(z_pair, pair_mask, dz_out, ln_in, w_proj, b_proj, ln_mid, w_out, b_out):
        mask = pair_mask[0].reshape(64, 2, 2, 64).transpose(0, 2, 1, 3).reshape(64, N).astype(F32)

        prm = jnp.concatenate([ln_in, ln_mid, b_out[:, None], b_proj.reshape(2, 5, C)], axis=1).astype(F32)
        prm = jnp.broadcast_to(prm[..., None], (2, 10, C, N))
        wt = jnp.swapaxes(w_proj, 1, 2)
        wot = jnp.swapaxes(w_out, 1, 2)

        def pick(k, *shape):
            return pl.BlockSpec((None,) + shape, lambda i: (k,) + (0,) * len(shape))

        def vecs(k, n, at):
            return pl.BlockSpec((None, n, C, N), lambda i: (k, at, 0, 0))

        def ln_s(k):
            return [vecs(k, 2, 0)]

        def mid_s(k):
            return [vecs(k, 2, 1)]

        def bias_s(k):
            return [pl.BlockSpec((None, None, C, N), lambda i: (k, 4, 0, 0))]

        def proj_s(k):
            return [pick(k, 640, C)]

        def bp_s(k):
            return [vecs(k, 5, 1)]

        same = lambda i: i
        cm_all = sds((C, 128, N), BF16)
        cm_full = sds((C, N, N), BF16)
        cm_own = sds((C, 64, N), BF16)
        rt_all = sds((128, C, N), BF16)
        rt_f32 = sds((128, C, N), F32)
        rt_own = sds((64, C, N), BF16)
        vm = pl.BlockSpec(memory_space=pltpu.VMEM)

        a0, zh0, zt0, g0, mask_all, a0f, b0f = call(
            pre_kernel, 8, [ANY, vm] + ln_s(0) + proj_s(0) + bp_s(0),
            [cm_spec(rb), rows_spec((C, N), rb), rows_spec((C, N), rb), rows_spec((C, N), rb), vm, ANY, ANY],
            [cm_all, rt_all, rt_all, rt_f32, sds((128, N), F32), cm_full, cm_full],
            [scr(), scr(), pltpu.VMEM((128, N), F32), pltpu.VMEM((128, N, C), BF16)] + [pltpu.SemaphoreType.DMA((4,))] * 3 + [pltpu.SemaphoreType.DMA((3,))] + ship_scratch() * 2,
            "pre", 1)(z_pair[0], mask, prm, wt, prm)
        dz_own, a0 = lax.optimization_barrier((dz_out[0], a0))
        dz_oth = lax.ppermute(dz_own, "dap", SWAP_X)
        x0 = jnp.einsum("cik,cjk->cij", a0, b0f, preferred_element_type=F32)

        zm, zh1, g1, a1o, b1o, a1c, b1f = call(
            mid_kernel, 8,
            [cm_spec(rb), rows_spec((C, N), rb), rows_spec((C, N), rb), rows_spec((N,), rb)] + mid_s(0) + [pick(0, C, C)] + bias_s(0) + ln_s(1) + proj_s(1) + bp_s(1),
            [rows_spec((C, N), rb), rows_spec((C, N), rb), rows_spec((C, N), rb), cm_spec(first4), cm_spec(first4), ANY, ANY],
            [rt_all, rt_all, rt_f32, cm_own, cm_own, sds((C, N, 128), BF16), cm_full],
            [scr(), scr(), scr()] + ship_scratch() * 2,
            "mid", 2)(x0, g0, zt0, mask_all, prm, wot, prm, prm, wt, prm)
        x1 = jnp.einsum("cki,ckj->cij", a1c, b1f, preferred_element_type=F32)

        late = lambda i: lax.max(i - 4, 0)
        smb = lambda k: mid_s(k) + [pick(k, C, C), pick(k, C, C)] + bias_s(k)
        zo, dpg1, dzt, dwo1, vec1, dx1f = call(
            post1_kernel, 8,
            [cm_spec(rb), rows_spec((C, N), rb), rows_spec((C, N), rb), rows_spec((N, C), first4), rows_spec((N, C), late)] + smb(1),
            [rows_spec((C, N), first4), rows_spec((C, N), first4), rows_spec((C, N), first4), full((C, C)), full((4, C, C)), ANY],
            [rt_own, rt_own, rt_own, sds((C, C), F32), sds((4, C, C), F32), cm_full],
            [scr(), scr()] + ship_scratch(), "post1", 3)(
            x1, g1, zm, dz_own, dz_oth, prm, wot, w_out, prm)
        da1 = jnp.einsum("ckj,cij->cki", b1o, dx1f, preferred_element_type=F32).astype(BF16)
        db1 = jnp.einsum("cki,cij->ckj", a1o, dx1f, preferred_element_type=F32).astype(BF16)

        own = lambda i: i + 4 * partner(1)[0]
        wp = lambda k: ln_s(k) + proj_s(k) + [pick(k, C, 640)] + bp_s(k)
        dzm, dx0, dpg0, dwp1, dwo0, vec2, vec3, dx0k = call(
            midb_kernel, 4,
            [cm_spec(same), cm_spec(same), rows_spec((C, N), own), rows_spec((C, N), own), rows_spec((N,), own),
             rows_spec((C, N), same), rows_spec((C, N), same), cm_spec(own), rows_spec((C, N), own)] + wp(1) + smb(0),
            [rows_spec((C, N), same), cm_spec(same), rows_spec((C, N), same), full((640, C)), full((C, C)), full((6, C, C)), full((4, C, C)), ANY],
            [rt_own, sds((C, 64, N), BF16), rt_own, sds((640, C), F32), sds((C, C), F32), sds((6, C, C), F32), sds((4, C, C), F32), sds((C, N, 128), BF16)],
            [scr(), scr(), scr(), scr(), pltpu.VMEM((640, GR * N), BF16), scr(), pltpu.VMEM((2, C, RB, N), BF16)]
            + [pltpu.SemaphoreType.DMA((k,)) for k in (2, 2, 4, 2, 4, 4, 4)], "midb", 4)(
            da1, db1, zh1, zm, mask_all, dpg1, dzt, x0, g0, prm, wt, w_proj, prm,
            prm, wot, w_out, prm)
        da0 = jnp.einsum("cij,cjk->cik", dx0, b0f, preferred_element_type=F32).astype(BF16)
        db0 = jnp.einsum("cij,cik->cjk", dx0k, a0f, preferred_element_type=F32).astype(BF16)

        dzp, zo, dwp0, vec4 = call(
            last_kernel, 4,
            [cm_spec(same), cm_spec(lambda i: i + 4 * partner(0)[0]), rows_spec((C, N), own), rows_spec((C, N), own), rows_spec((N,), own),
             rows_spec((C, N), same), rows_spec((C, N), same), rows_spec((C, N), same)] + wp(0),
            [rows_spec((N, C), same), rows_spec((N, C), same), full((640, C)), full((6, C, C))],
            [sds((64, N, C), BF16), sds((64, N, C), BF16), sds((640, C), F32), sds((6, C, C), F32)],
            [scr(), scr(), pltpu.VMEM((640, GR * N), BF16)], "last")(
            da0, db0, zh0, zt0, mask_all, dpg0, dzm, zo, prm, wt, w_proj, prm)

        g = reduce_all(dwp0, dwo0, vec4, vec3, dwp1, dwo1, vec2, vec1)[:1568].reshape(2, 784, C)
        d_b = jnp.concatenate([g[:, 768:772].reshape(2, 512), g[:, 777]], axis=1)
        return (zo[None], dzp[None], g[:, 772:774], jnp.swapaxes(g[:, :640], 1, 2), d_b, g[:, 775:777], g[:, 640:768], g[:, 774])

    row_spec = P("dp", "dap")
    return jax.shard_map(local_step, mesh=mesh, in_specs=(row_spec, row_spec, row_spec, P(), P(), P(), P(), P(), P()), out_specs=(row_spec, row_spec, P(), P(), P(), P(), P(), P()), check_vma=False)
```

```python
import functools
import jax
import jax.numpy as jnp
from jax import lax
from jax.experimental import pallas as pl
from jax.experimental.pallas import tpu as pltpu
from jax.sharding import PartitionSpec as P

LN_EPS = 1e-5
RB = 16
SP = 17
UN = 16
GR = 8
CB = 16
DZ1 = 48
F32 = jnp.float32
BF16 = jnp.bfloat16
C = 128
N = 256
HB = 64
CP = 640
SWAP_X = [(0, 2), (2, 0), (1, 3), (3, 1)]


def dot(a, b):
    return lax.dot_general(a, b, (((1,), (0,)), ((), ())), preferred_element_type=F32)


def dot_t(a, b):
    return dot(a, jnp.transpose(b))


def sig(v):
    return 0.5 * jnp.tanh(0.5 * v) + 0.5


def norm(v):
    mu = jnp.mean(v, axis=0, keepdims=True)
    vc = v - mu
    rstd = lax.rsqrt(jnp.mean(vc * vc, axis=0, keepdims=True) + LN_EPS)
    return vc * rstd, rstd


def norm_bwd(d_hat, vn, rstd, gain):
    dn = d_hat * gain
    m1 = jnp.mean(dn, axis=0, keepdims=True)
    m2 = jnp.mean(dn * vn, axis=0, keepdims=True)
    return rstd * (dn - m1 - vn * m2)


def perm_cols(t):
    return jnp.concatenate([t[0:HB], t[C:192], t[HB:C], t[192:N]], axis=0)


def load_t(ref, r):
    return jnp.transpose(perm_cols(ref[r])).astype(F32)


def store_t(ref, r, val):
    ref[r] = perm_cols(jnp.transpose(val))


def by_chip(v):
    v0, v1 = v[:, :C], v[:, C:]
    low = lax.broadcasted_iota(jnp.int32, (C, C), 1) < HB
    return jnp.concatenate([jnp.where(low, v0, pltpu.roll(v1, HB, 1)), jnp.where(low, pltpu.roll(v0, HB, 1), v1)], axis=1)


def put_row(scr, r, val):
    for h in range(2):
        scr[h, pl.ds(r, C, stride=SP), :] = val[:, h * C:(h + 1) * C]


def get_row(scr, r):
    return jnp.concatenate([scr[h, pl.ds(r, C, stride=SP), :] for h in range(2)], axis=1)


def pack(scr, out_ref):
    def body(i, _):
        c0 = i * 8
        for k in range(8):
            for h in range(2):
                out_ref[c0 + k, :, h * C:(h + 1) * C] = scr[h, pl.ds((c0 + k) * SP, RB), :].astype(out_ref.dtype)
        return 0
    lax.fori_loop(0, C // 8, body, 0)


def unpack(in_ref, scr):
    def body(i, _):
        c0 = i * 8
        for k in range(8):
            for h in range(2):
                scr[h, pl.ds((c0 + k) * SP, RB), :] = in_ref[c0 + k, :, h * C:(h + 1) * C].astype(F32)
        return 0
    lax.fori_loop(0, C // 8, body, 0)


def gates(zh, m, wt, bp, scr_a, scr_b, g_ref, r):
    p = dot(wt[...], zh)
    put_row(scr_a, r, sig(p[0:C] + bp[0]) * (p[C:N] + bp[1]) * m)
    put_row(scr_b, r, sig(p[N:384] + bp[2]) * (p[384:512] + bp[3]) * m)
    g_ref[r] = sig(p[512:CP] + bp[4])


def groups(body):
    lax.fori_loop(0, RB // GR, body, 0)


def halves(v):
    return v[:, :C] + v[:, C:]


CHUNKS = ((0, CP, (0, 1, 2, 3)), (CP, 512, (0, 2, 3, 1)), (1152, 512, (0, 3, 1, 2)))
GROWS = 1664


def coords():
    return lax.axis_index("dp"), lax.axis_index("dap")


def partner(k):
    dp, dap = coords()
    if k < 2:
        bit = lax.rem(dap // (1 << k), 2)
        return bit, (dp, dap + (1 << k) * (1 - 2 * bit))
    bit = lax.rem(dp // (1 << (k - 2)), 2)
    return bit, (dp + (1 << (k - 2)) * (1 - 2 * bit), dap)


def greet(keys):
    barrier = pltpu.get_barrier_semaphore()
    for k in keys:
        pl.semaphore_signal(barrier, inc=1, device_id=partner(k)[1], device_id_type=pl.DeviceIdType.MESH)
    pl.semaphore_wait(barrier, len(keys))


def remote(src, dst, send, recv, k):
    return pltpu.make_async_remote_copy(src_ref=src, dst_ref=dst, send_sem=send, recv_sem=recv, device_id=partner(k)[1], device_id_type=pl.DeviceIdType.MESH)


def rb(i):
    return lax.rem(i + 4 * partner(1)[0], 8)


def first4(i):
    return lax.min(i, 3)


def pair_parts(step, st, out, split):
    bit = partner(0)[0]
    slot = lax.rem(step, 2)
    dst = out.at[:, pl.ds(pl.multiple_of(bit * C + rb(step) * RB, RB), RB), :]
    mine = theirs = st.at[slot]
    if split:
        mine = st.at[slot, :, :, pl.ds(pl.multiple_of(bit * C, C), C)]
        theirs = st.at[slot, :, :, pl.ds(pl.multiple_of((1 - bit) * C, C), C)]
    return slot, dst, mine, theirs


def pair_here(step, st, out, sems, split):
    slot, dst, mine, _ = pair_parts(step, st, out, split)
    return pltpu.make_async_copy(mine, dst, sems[0].at[slot])


def pair_there(step, st, out, sems, split):
    slot, dst, _, theirs = pair_parts(step, st, out, split)
    return remote(theirs, dst, sems[1].at[slot], sems[2].at[step], 0)


def ship(step, items):
    @pl.when(step >= 2)
    def _():
        for _, *it in items:
            pair_here(step - 2, *it).wait()
            pair_there(step - 2, *it).wait_send()
    for scr, *it in items:
        pack(scr, it[0].at[lax.rem(step, 2)])
        pair_here(step, *it).start()
        pair_there(step, *it).start()

    @pl.when(step == 7)
    def _():
        for _, *it in items:
            for k in (6, 7):
                pair_here(k, *it).wait()
                pair_there(k, *it).wait_send()
            for k in range(8):
                pair_there(k, *it).wait_recv()


def ship_scratch():
    return [pltpu.VMEM((2, C, RB, N), BF16), pltpu.SemaphoreType.DMA((2,)), pltpu.SemaphoreType.DMA((2,)), pltpu.SemaphoreType.DMA((8,))]


def pre_kernel(z_ref, dz_ref, m_ref, ln_ref, wt_ref, bp_ref, a_ref, zh_ref, zt_ref, g_ref, mall_ref, af_ref, bf_ref, dzs_ref,
               scr_a, scr_b, dzbuf, dzsem, mbuf, zbuf, zloc, zsend, zrecv, msem, st_a, la, sa, ra, st_b, lb, sb, rb_):
    step = pl.program_id(0)
    xb = partner(1)[0]

    def z_here(q):
        return pltpu.make_async_copy(z_ref.at[pl.ds(q * RB, RB)], zbuf.at[pl.ds(q * RB, RB)], zloc.at[q])

    def z_there(q):
        return remote(z_ref.at[pl.ds(q * RB, RB)], zbuf.at[pl.ds(HB + q * RB, RB)], zsend.at[q], zrecv.at[q], 1)

    def dz_in():
        return pltpu.make_async_copy(dz_ref.at[pl.ds(0, DZ1)], dzbuf, dzsem.at[0])

    def dz_out():
        return pltpu.make_async_copy(dzbuf, dzs_ref, dzsem.at[1])

    @pl.when(step == 1)
    def _():
        dz_in().start()

    @pl.when(step == 3)
    def _():
        dz_in().wait()
        dz_out().start()

    @pl.when(step == 6)
    def _():
        dz_out().wait()

    m_dst = mbuf.at[pl.ds(pl.multiple_of(xb * HB, HB), HB), :]

    def m_there():
        return remote(m_ref, m_dst, msem.at[1], msem.at[2], 1)

    @pl.when(step == 0)
    def _():
        for q in range(4):
            z_here(q).start()
        greet((0, 1))
        m_here = pltpu.make_async_copy(m_ref, m_dst, msem.at[0])
        m_here.start()
        m_there().start()
        for q in range(4):
            z_there(q).start()
        m_here.wait()
    for q in range(4):
        @pl.when(step == q)
        def _():
            z_here(q).wait()

        @pl.when(step == 4 + q)
        def _():
            if q == 0:
                m_there().wait()
            z_there(q).wait()

    def row(r, _):
        zt = load_t(zbuf, step * RB + r)
        zt_ref[r] = zt.astype(BF16)
        zn, _ = norm(zt)
        zh = (zn * ln_ref[0] + ln_ref[1]).astype(BF16)
        zh_ref[r] = zh
        gates(zh, mbuf[pl.ds(rb(step) * RB + r, 1), :], wt_ref, bp_ref, scr_a, scr_b, g_ref, r)
        return 0
    lax.fori_loop(0, RB, row, 0, unroll=UN)
    ship(step, [(scr_a, st_a, af_ref, (la, sa, ra), False), (scr_b, st_b, bf_ref, (lb, sb, rb_), False)])
    a_ref[...] = st_a[lax.rem(step, 2)]

    @pl.when(step == 7)
    def _():
        mall_ref[...] = mbuf[...]


def mid_kernel(x_ref, g_ref, zt_ref, m_ref, lnm_ref, wot_ref, bo_ref, ln_ref, wt_ref, bp_ref,
               zm_ref, zh1_ref, g1_ref, ao_ref, bo1_ref, ac_ref, bf_ref, scr_x, scr_a, scr_b, st_a, la, sa, ra, st_b, lb, sb, rb_):
    step = pl.program_id(0)

    @pl.when(step == 0)
    def _():
        greet((0,))
    unpack(x_ref, scr_x)

    def row(r, _):
        xn, _ = norm(get_row(scr_x, r))
        xh = (xn * lnm_ref[0] + lnm_ref[1]).astype(BF16)
        u = dot(wot_ref[...], xh) + bo_ref[...]
        zm = (zt_ref[r].astype(F32) + g_ref[r] * u).astype(BF16)
        zm_ref[r] = zm
        zn, _ = norm(zm.astype(F32))
        zh = (zn * ln_ref[0] + ln_ref[1]).astype(BF16)
        zh1_ref[r] = zh
        gates(zh, m_ref[pl.ds(r, 1), :], wt_ref, bp_ref, scr_a, scr_b, g1_ref, r)
        return 0
    lax.fori_loop(0, RB, row, 0, unroll=UN)
    ship(step, [(scr_a, st_a, ac_ref, (la, sa, ra), True), (scr_b, st_b, bf_ref, (lb, sb, rb_), False)])

    @pl.when(step < 4)
    def _():
        ao_ref[...] = st_a[lax.rem(step, 2)]
        bo1_ref[...] = st_b[lax.rem(step, 2)]


def post_row(x, g, lnm_ref, wot_ref, wo_ref, bo_ref, dz):
    xn, rstd = norm(x)
    xh = (xn * lnm_ref[0] + lnm_ref[1]).astype(BF16)
    u = dot(wot_ref[...], xh) + bo_ref[...]
    d_pg = dz * u * (g * (1.0 - g))
    d_upd = dz * g
    d_bf = d_upd.astype(BF16)
    d_xh = dot(wo_ref[...], d_bf)
    dx = norm_bwd(d_xh, xn, rstd, lnm_ref[0])
    return xh, xn, u, d_pg, d_upd, d_bf, d_xh, dx


def post_vecs(vec_ref, d_upd, d_xh, xn, d_pg):
    for q, v in enumerate((d_upd, d_xh * xn, d_xh, d_pg)):
        vec_ref[q] += halves(v)


def add_outer(acc_ref, left, right):
    acc_ref[...] += dot(jnp.concatenate(left, axis=1), jnp.transpose(jnp.concatenate(right, axis=1)))


def zero(*refs):
    for ref in refs:
        ref[...] = jnp.zeros_like(ref)


def post1_kernel(x_ref, g_ref, zm_ref, dz_ref, dzo_ref, dzall_ref, lnm_ref, wot_ref, wo_ref, bo_ref,
                 zo_ref, dpg_ref, dzt_ref, dwo_ref, vec_ref, dxf_ref, scr_x, scr_d, dzbuf, dzsem, st, lsem, ssem, rsem):
    step = pl.program_id(0)

    def dz_there():
        return remote(dzall_ref.at[pl.ds(DZ1, RB)], dzbuf.at[1], dzsem.at[0], dzsem.at[1], 1)

    @pl.when(step == 0)
    def _():
        greet((0, 1))
        dz_there().start()
        zero(dwo_ref, vec_ref)
    unpack(x_ref, scr_x)

    @pl.when((step >= 4) & (step < 7))
    def _():
        def copy_row(r, _):
            dzbuf[0, r] = dzo_ref[r]
            return 0
        lax.fori_loop(0, RB, copy_row, 0)

    @pl.when(step == 7)
    def _():
        dz_there().wait()

    @pl.when(step >= 4)
    def _():
        def row(r, _):
            dz = load_t(dzbuf.at[step // 7], r)
            res = post_row(get_row(scr_x, r), g_ref[r], lnm_ref, wot_ref, wo_ref, bo_ref, dz)
            put_row(scr_d, r, res[-1])
            return 0
        lax.fori_loop(0, RB, row, 0, unroll=GR)

    @pl.when(step < 4)
    def _():
        def group(i, _):
            left, right = [], []
            for k in range(GR):
                r = i * GR + k
                dz = load_t(dz_ref, r)
                dzt_ref[r] = dz.astype(BF16)
                g = g_ref[r]
                xh, xn, u, d_pg, d_upd, d_bf, d_xh, dx = post_row(get_row(scr_x, r), g, lnm_ref, wot_ref, wo_ref, bo_ref, dz)
                put_row(scr_d, r, dx)
                dpg_ref[r] = d_pg.astype(BF16)
                zo_ref[r] = (zm_ref[r].astype(F32) + g * u).astype(BF16)
                post_vecs(vec_ref, d_upd, d_xh, xn, d_pg)
                left.append(xh)
                right.append(d_bf)
            add_outer(dwo_ref, left, right)
            return 0
        groups(group)
    ship(step, [(scr_d, st, dxf_ref, (lsem, ssem, rsem), False)])


def pre_bwd_row(r, k, z, zh, m, d_pg, scr_a, scr_b, ln_ref, wt_ref, w_ref, bp_ref, dp_ref, vec_ref):
    p = dot(wt_ref[0:512, :], zh)
    cols = slice(k * N, k * N + N)
    for q, scr in ((0, scr_a), (1, scr_b)):
        s = sig(p[q * N:q * N + C] + bp_ref[2 * q])
        v = p[q * N + C:q * N + N] + bp_ref[2 * q + 1]
        d_s = get_row(scr, r) * m
        d_v = d_s * s
        d_g = d_v * v * (1.0 - s)
        dp_ref[q * N:q * N + C, cols] = d_g.astype(BF16)
        dp_ref[q * N + C:q * N + N, cols] = d_v.astype(BF16)
        vec_ref[2 * q] += halves(d_g)
        vec_ref[2 * q + 1] += halves(d_v)
    dp_ref[512:CP, cols] = d_pg
    d_zh = dot(w_ref[...], dp_ref[:, cols])
    zn, rstd = norm(z)
    vec_ref[4] += halves(d_zh * zn)
    vec_ref[5] += halves(d_zh)
    return norm_bwd(d_zh, zn, rstd, ln_ref[0])


def midb_kernel(da_ref, db_ref, zh1_ref, zm_ref, m_ref, dpg1_ref, dzt_ref, x0_ref, g0_ref,
                ln_ref, wt_ref, w_ref, bp_ref, lnm_ref, wot_ref, wo_ref, bo_ref,
                dzm_ref, dx_ref, dpg0_ref, dwp_ref, dwo_ref, vec_ref, vec2_ref, dxk_ref, scr_a, scr_b, scr_x, scr_d, dp_ref,
                scr_e, st, lsem, csend, crecv, xsend, xrecv, rsend, rrecv):
    step = pl.program_id(0)
    cbit = partner(0)[0]
    xbit = partner(1)[0]

    def block(core, chip, k):
        return dxk_ref.at[:, pl.ds(pl.multiple_of(core * C + chip * HB + k * RB, RB), RB), :]

    def part(k, chip):
        return st.at[lax.rem(k, 2), :, :, pl.ds(pl.multiple_of(chip * C, C), C)]

    def here(k):
        return pltpu.make_async_copy(part(k, xbit), block(cbit, xbit, k), lsem.at[lax.rem(k, 2)])

    def to_core(k):
        return remote(part(k, xbit), block(cbit, xbit, k), csend.at[lax.rem(k, 2)], crecv.at[k], 0)

    def to_chip(k):
        return remote(part(k, 1 - xbit), block(cbit, xbit, k), xsend.at[lax.rem(k, 2)], xrecv.at[k], 1)

    def relay(k):
        blk = block(cbit, 1 - xbit, k)
        return remote(blk, blk, rsend.at[k], rrecv.at[k], 0)

    def settle(k):
        here(k).wait()
        to_core(k).wait_send()
        to_chip(k).wait_send()

    @pl.when(step == 0)
    def _():
        greet((0, 1))
        zero(dwp_ref, dwo_ref, vec_ref, vec2_ref)
    unpack(da_ref, scr_a)
    unpack(db_ref, scr_b)
    unpack(x0_ref, scr_x)

    def group(i, _):
        left, right, zhs = [], [], []
        for k in range(GR):
            r = i * GR + k
            zh = zh1_ref[r]
            zhs.append(zh)
            dz_norm = pre_bwd_row(r, k, zm_ref[r].astype(F32), zh, m_ref[pl.ds(r, 1), :], dpg1_ref[r], scr_a, scr_b,
                                  ln_ref, wt_ref, w_ref, bp_ref, dp_ref, vec_ref)
            dzm = (dzt_ref[r].astype(F32) + dz_norm).astype(BF16)
            dzm_ref[r] = dzm
            xh, xn, u, d_pg, d_upd, d_bf, d_xh, dx = post_row(get_row(scr_x, r), g0_ref[r], lnm_ref, wot_ref, wo_ref, bo_ref, dzm.astype(F32))
            put_row(scr_d, r, dx)
            put_row(scr_e, r, by_chip(dx))
            dpg0_ref[r] = d_pg.astype(BF16)
            post_vecs(vec2_ref, d_upd, d_xh, xn, d_pg)
            left.append(xh)
            right.append(d_bf)
        add_outer(dwo_ref, left, right)
        add_outer(dwp_ref, [dp_ref[...]], zhs)
        return 0
    groups(group)

    @pl.when(step >= 2)
    def _():
        settle(step - 2)
    pack(scr_e, st.at[lax.rem(step, 2)])
    to_chip(step).start()
    to_core(step).start()
    here(step).start()
    pack(scr_d, dx_ref)

    @pl.when(step >= 2)
    def _():
        to_chip(step - 2).wait_recv()
        relay(step - 2).start()

    @pl.when(step == 3)
    def _():
        for k in (2, 3):
            to_chip(k).wait_recv()
            relay(k).start()
            settle(k)
        for k in range(4):
            to_core(k).wait_recv()
            relay(k).wait()


def last_kernel(da_ref, db_ref, zh_ref, zt_ref, m_ref, dpg_ref, dzm_ref, zo_ref, ln_ref, wt_ref, w_ref, bp_ref,
                dz_ref, zout_ref, dwp_ref, vec_ref, scr_a, scr_b, dp_ref):
    @pl.when(pl.program_id(0) == 0)
    def _():
        zero(dwp_ref, vec_ref)
    unpack(da_ref, scr_a)
    unpack(db_ref, scr_b)

    def group(i, _):
        zhs = []
        for k in range(GR):
            r = i * GR + k
            zh = zh_ref[r]
            zhs.append(zh)
            dz_norm = pre_bwd_row(r, k, zt_ref[r].astype(F32), zh, m_ref[pl.ds(r, 1), :], dpg_ref[r], scr_a, scr_b,
                                  ln_ref, wt_ref, w_ref, bp_ref, dp_ref, vec_ref)
            store_t(dz_ref, r, (dzm_ref[r].astype(F32) + dz_norm).astype(BF16))
            store_t(zout_ref, r, zo_ref[r])
        add_outer(dwp_ref, [dp_ref[...]], zhs)
        return 0
    groups(group)


def grads1_kernel(a_ref, b_ref, dx_ref, da_ref, db_ref):
    for k in range(CB):
        dx = dx_ref[k]
        da_ref[k] = dot(b_ref[k], jnp.transpose(dx)).astype(BF16)
        db_ref[k] = dot(a_ref[k], dx).astype(BF16)


def grads0_kernel(dx_ref, b_ref, dxk_ref, a_ref, da_ref, db_ref, turned):
    own = pl.ds(pl.multiple_of(partner(0)[0] * HB, HB), HB)
    for k in range(CB):
        turned[k] = jnp.transpose(dxk_ref[k])
        da_ref[k] = dot(dx_ref[k], b_ref[k]).astype(BF16)
    for k in range(CB):
        db_ref[k] = dot(turned[k, own, :], a_ref[k]).astype(BF16)


def sds(shape, dtype):
    return jax.ShapeDtypeStruct(shape, dtype)


def full(shape):
    nd = len(shape)
    return pl.BlockSpec(shape, lambda *_: (0,) * nd)


def rows_spec(shape, fn):
    return pl.BlockSpec((RB,) + shape, lambda i: (fn(i),) + (0,) * len(shape))


def cm_spec(fn):
    return pl.BlockSpec((C, RB, N), lambda i: (0, fn(i), 0))


def scr():
    return pltpu.VMEM((2, C * SP, C), F32)


ANY = pl.BlockSpec(memory_space=pl.ANY)


def call(kernel, grid, in_specs, out_specs, out_shape, scratch, name, cid=None):
    return pl.pallas_call(
        kernel, name=name, out_shape=out_shape, grid=(grid,), in_specs=in_specs, out_specs=out_specs, scratch_shapes=scratch,
        compiler_params=pltpu.CompilerParams(dimension_semantics=("arbitrary",), vmem_limit_bytes=60 << 20, collective_id=cid, has_side_effects=cid is not None))


def reduce_kernel(dwp0_ref, dwo0_ref, pre0_ref, post0_ref, dwp1_ref, dwo1_ref, pre1_ref, post1_ref, out_ref, acc, got0, got1, got2, got3, send, recv):
    greet((0, 1, 2, 3))
    parts = ((dwp0_ref, dwo0_ref, pre0_ref, post0_ref), (dwp1_ref, dwo1_ref, pre1_ref, post1_ref))
    for k, (dwp, dwo, vpre, vpost) in enumerate(parts):
        acc[784 * k:784 * k + CP, :] = dwp[...]
        acc[784 * k + CP:784 * k + 768, :] = dwo[...]
        rows = [jnp.sum(jnp.transpose(v[q]), axis=0, keepdims=True) for v, n in ((vpre, 6), (vpost, 4)) for q in range(n)]
        acc[784 * k + 768:784 * k + 784, :] = jnp.concatenate(rows + [jnp.zeros((6, C), F32)], axis=0)
    acc[1568:GROWS, :] = jnp.zeros((GROWS - 1568, C), F32)
    got = (got0, got1, got2, got3)
    spans = [[r0, n] for r0, n, _ in CHUNKS]
    for st in range(4):
        copies = []
        base = 0
        for ch, (_, _, order) in enumerate(CHUNKS):
            lo, n = spans[ch]
            half = n // 2
            bit = partner(order[st])[0]
            give = pl.multiple_of(lo + (1 - bit) * half, 8)
            keep = pl.multiple_of(lo + bit * half, 8)
            land = got[st].at[pl.ds(base, half), :]
            cp = remote(acc.at[pl.ds(give, half), :], land, send.at[st, ch], recv.at[st, ch], order[st])
            cp.start()
            copies.append((cp, keep, half, base))
            spans[ch] = [keep, half]
            base += half
        for cp, keep, half, base in copies:
            cp.wait()
            acc[pl.ds(keep, half), :] += got[st][base:base + half, :]
    for lo, n in spans:
        out_ref[pl.ds(lo, n), :] = acc[pl.ds(lo, n), :]
    for st in (3, 2, 1, 0):
        copies = []
        for ch, (_, _, order) in enumerate(CHUNKS):
            lo, n = spans[ch]
            bit = partner(order[st])[0]
            seg = out_ref.at[pl.ds(pl.multiple_of(lo, 8), n), :]
            cp = remote(seg, seg, send.at[4 + st, ch], recv.at[4 + st, ch], order[st])
            cp.start()
            copies.append(cp)
            spans[ch] = [lo - bit * n, 2 * n]
        for cp in copies:
            cp.wait()


def reduce_all(*g):
    vm = pl.BlockSpec(memory_space=pltpu.VMEM)
    return pl.pallas_call(
        reduce_kernel, name="reduce", out_shape=sds((GROWS, C), F32), in_specs=[vm] * 8, out_specs=vm,
        scratch_shapes=[pltpu.VMEM((GROWS, C), F32)] + [pltpu.VMEM((GROWS >> (k + 1), C), F32) for k in range(4)]
        + [pltpu.SemaphoreType.DMA((8, 3)), pltpu.SemaphoreType.DMA((8, 3))],
        compiler_params=pltpu.CompilerParams(collective_id=0, has_side_effects=True))(*g)


def solution(mesh):
    def local_step(z_pair, pair_mask, dz_out, ln_in, w_proj, b_proj, ln_mid, w_out, b_out):
        mask = pair_mask[0].reshape(HB, 2, 2, HB).transpose(0, 2, 1, 3).reshape(HB, N).astype(F32)

        prm = jnp.concatenate([ln_in, ln_mid, b_out[:, None], b_proj.reshape(2, 5, C)], axis=1).astype(F32)
        prm = jnp.broadcast_to(prm[..., None], (2, 10, C, N))
        wt = jnp.swapaxes(w_proj, 1, 2)
        wot = jnp.swapaxes(w_out, 1, 2)

        def pick(k, *shape):
            return pl.BlockSpec((None,) + shape, lambda i: (k,) + (0,) * len(shape))

        def vecs(k, n, at):
            return pl.BlockSpec((None, n, C, N), lambda i: (k, at, 0, 0))

        def ln_s(k):
            return [vecs(k, 2, 0)]

        def mid_s(k):
            return [vecs(k, 2, 1)]

        def bias_s(k):
            return [pl.BlockSpec((None, None, C, N), lambda i: (k, 4, 0, 0))]

        def proj_s(k):
            return [pick(k, CP, C)]

        def bp_s(k):
            return [vecs(k, 5, 1)]

        same = lambda i: i
        cm_all = sds((C, C, N), BF16)
        cm_full = sds((C, N, N), BF16)
        cm_own = sds((C, HB, N), BF16)
        rt_all = sds((C, C, N), BF16)
        rt_f32 = sds((C, C, N), F32)
        rt_own = sds((HB, C, N), BF16)
        vm = pl.BlockSpec(memory_space=pltpu.VMEM)

        a0, zh0, zt0, g0, mask_all, a0f, b0f, dz_head = call(
            pre_kernel, 8, [ANY, ANY, vm] + ln_s(0) + proj_s(0) + bp_s(0),
            [cm_spec(rb), rows_spec((C, N), rb), rows_spec((C, N), rb), rows_spec((C, N), rb), vm, ANY, ANY, ANY],
            [cm_all, rt_all, rt_all, rt_f32, sds((C, N), F32), cm_full, cm_full, sds((DZ1, N, C), BF16)],
            [scr(), scr(), pltpu.VMEM((DZ1, N, C), BF16), pltpu.SemaphoreType.DMA((2,)), pltpu.VMEM((C, N), F32), pltpu.VMEM((C, N, C), BF16)] + [pltpu.SemaphoreType.DMA((4,))] * 3 + [pltpu.SemaphoreType.DMA((3,))] + ship_scratch() * 2,
            "pre", 1)(z_pair[0], dz_out[0], mask, prm, wt, prm)
        dz_own = dz_out[0]
        dz_oth = lax.ppermute(dz_head, "dap", SWAP_X)
        x0 = jnp.einsum("cik,cjk->cij", a0, b0f, preferred_element_type=F32)

        zm, zh1, g1, a1o, b1o, a1c, b1f = call(
            mid_kernel, 8,
            [cm_spec(rb), rows_spec((C, N), rb), rows_spec((C, N), rb), rows_spec((N,), rb)] + mid_s(0) + [pick(0, C, C)] + bias_s(0) + ln_s(1) + proj_s(1) + bp_s(1),
            [rows_spec((C, N), rb), rows_spec((C, N), rb), rows_spec((C, N), rb), cm_spec(first4), cm_spec(first4), ANY, ANY],
            [rt_all, rt_all, rt_f32, cm_own, cm_own, sds((C, N, C), BF16), cm_full],
            [scr(), scr(), scr()] + ship_scratch() * 2,
            "mid", 2)(x0, g0, zt0, mask_all, prm, wot, prm, prm, wt, prm)
        x1 = jnp.einsum("cki,ckj->cij", a1c, b1f, preferred_element_type=F32)

        late = lambda i: lax.min(lax.max(i - 4, 0), 2)
        smb = lambda k: mid_s(k) + [pick(k, C, C), pick(k, C, C)] + bias_s(k)
        zo, dpg1, dzt, dwo1, vec1, dx1f = call(
            post1_kernel, 8,
            [cm_spec(rb), rows_spec((C, N), rb), rows_spec((C, N), rb), rows_spec((N, C), first4), rows_spec((N, C), late), ANY] + smb(1),
            [rows_spec((C, N), first4), rows_spec((C, N), first4), rows_spec((C, N), first4), full((C, C)), full((4, C, C)), ANY],
            [rt_own, rt_own, rt_own, sds((C, C), F32), sds((4, C, C), F32), cm_full],
            [scr(), scr(), pltpu.VMEM((2, RB, N, C), BF16), pltpu.SemaphoreType.DMA((2,))] + ship_scratch(), "post1", 3)(
            x1, g1, zm, dz_own, dz_oth, dz_own, prm, wot, w_out, prm)
        chan = lambda *sh: pl.BlockSpec((CB,) + sh, lambda i: (i, 0, 0))
        da1, db1 = call(grads1_kernel, C // CB, [chan(HB, N), chan(HB, N), chan(N, N)], [chan(HB, N)] * 2, [cm_own] * 2, [], "grads1")(a1o, b1o, dx1f)

        own = lambda i: i + 4 * partner(1)[0]
        wp = lambda k: ln_s(k) + proj_s(k) + [pick(k, C, CP)] + bp_s(k)
        dzm, dx0, dpg0, dwp1, dwo0, vec2, vec3, dx0k = call(
            midb_kernel, 4,
            [cm_spec(same), cm_spec(same), rows_spec((C, N), own), rows_spec((C, N), own), rows_spec((N,), own),
             rows_spec((C, N), same), rows_spec((C, N), same), cm_spec(own), rows_spec((C, N), own)] + wp(1) + smb(0),
            [rows_spec((C, N), same), cm_spec(same), rows_spec((C, N), same), full((CP, C)), full((C, C)), full((6, C, C)), full((4, C, C)), ANY],
            [rt_own, sds((C, HB, N), BF16), rt_own, sds((CP, C), F32), sds((C, C), F32), sds((6, C, C), F32), sds((4, C, C), F32), sds((C, N, C), BF16)],
            [scr(), scr(), scr(), scr(), pltpu.VMEM((CP, GR * N), BF16), scr(), pltpu.VMEM((2, C, RB, N), BF16)]
            + [pltpu.SemaphoreType.DMA((k,)) for k in (2, 2, 4, 2, 4, 4, 4)], "midb", 4)(
            da1, db1, zh1, zm, mask_all, dpg1, dzt, x0, g0, prm, wt, w_proj, prm,
            prm, wot, w_out, prm)
        da0, db0 = call(grads0_kernel, C // CB, [chan(HB, N), chan(N, N), chan(N, C), chan(N, N)], [chan(HB, N)] * 2, [cm_own] * 2,
                        [pltpu.VMEM((CB, C, N), BF16)], "grads0")(dx0, b0f, dx0k, a0f)

        dzp, zo, dwp0, vec4 = call(
            last_kernel, 4,
            [cm_spec(same), cm_spec(same), rows_spec((C, N), own), rows_spec((C, N), own), rows_spec((N,), own),
             rows_spec((C, N), same), rows_spec((C, N), same), rows_spec((C, N), same)] + wp(0),
            [rows_spec((N, C), same), rows_spec((N, C), same), full((CP, C)), full((6, C, C))],
            [sds((HB, N, C), BF16), sds((HB, N, C), BF16), sds((CP, C), F32), sds((6, C, C), F32)],
            [scr(), scr(), pltpu.VMEM((CP, GR * N), BF16)], "last")(
            da0, db0, zh0, zt0, mask_all, dpg0, dzm, zo, prm, wt, w_proj, prm)

        g = reduce_all(dwp0, dwo0, vec4, vec3, dwp1, dwo1, vec2, vec1)[:1568].reshape(2, 784, C)
        d_b = jnp.concatenate([g[:, 768:772].reshape(2, 512), g[:, 777]], axis=1)
        return (zo[None], dzp[None], g[:, 772:774], jnp.swapaxes(g[:, :CP], 1, 2), d_b, g[:, 775:777], g[:, CP:768], g[:, 774])

    row_spec = P("dp", "dap")
    return jax.shard_map(local_step, mesh=mesh, in_specs=(row_spec, row_spec, row_spec, P(), P(), P(), P(), P(), P()), out_specs=(row_spec, row_spec, P(), P(), P(), P(), P(), P()), check_vma=False)
```

```python
import functools
import jax
import jax.numpy as jnp
from jax import lax
from jax.experimental import pallas as pl
from jax.experimental.pallas import tpu as pltpu
from jax.sharding import PartitionSpec as P

LN_EPS = 1e-5
RB = 16
SP = 17
UN = 16
GR = 8
CB = 16
DZ1 = 48
F32 = jnp.float32
BF16 = jnp.bfloat16
C = 128
N = 256
HB = 64
CP = 640
SWAP_X = [(0, 2), (2, 0), (1, 3), (3, 1)]


def dot(a, b):
    return lax.dot_general(a, b, (((1,), (0,)), ((), ())), preferred_element_type=F32)


def dot_t(a, b):
    return dot(a, jnp.transpose(b))


def sig(v):
    return 0.5 * jnp.tanh(0.5 * v) + 0.5


def norm(v):
    mu = jnp.mean(v, axis=0, keepdims=True)
    vc = v - mu
    rstd = lax.rsqrt(jnp.mean(vc * vc, axis=0, keepdims=True) + LN_EPS)
    return vc * rstd, rstd


def norm_bwd(d_hat, vn, rstd, gain):
    dn = d_hat * gain
    m1 = jnp.mean(dn, axis=0, keepdims=True)
    m2 = jnp.mean(dn * vn, axis=0, keepdims=True)
    return rstd * (dn - m1 - vn * m2)


def perm_cols(t):
    return jnp.concatenate([t[0:HB], t[C:192], t[HB:C], t[192:N]], axis=0)


def load_t(ref, r):
    return jnp.transpose(perm_cols(ref[r])).astype(F32)


def store_t(ref, r, val):
    ref[r] = perm_cols(jnp.transpose(val))


def by_chip(v):
    rows = v.shape[0]
    v0, v1 = v[:, :C], v[:, C:]
    low = lax.broadcasted_iota(jnp.int32, (rows, C), 1) < HB
    return jnp.concatenate([jnp.where(low, v0, pltpu.roll(v1, HB, 1)), jnp.where(low, pltpu.roll(v0, HB, 1), v1)], axis=1)


def put_row(scr, r, val):
    for h in range(2):
        scr[h, pl.ds(r, C, stride=SP), :] = val[:, h * C:(h + 1) * C]


def get_row(scr, r):
    return jnp.concatenate([scr[h, pl.ds(r, C, stride=SP), :] for h in range(2)], axis=1)


def pack(scr, out_ref):
    def body(i, _):
        c0 = i * 8
        for k in range(8):
            for h in range(2):
                out_ref[c0 + k, :, h * C:(h + 1) * C] = scr[h, pl.ds((c0 + k) * SP, RB), :].astype(out_ref.dtype)
        return 0
    lax.fori_loop(0, C // 8, body, 0)


def unpack(in_ref, scr):
    def body(i, _):
        c0 = i * 8
        for k in range(8):
            for h in range(2):
                scr[h, pl.ds((c0 + k) * SP, RB), :] = in_ref[c0 + k, :, h * C:(h + 1) * C].astype(F32)
        return 0
    lax.fori_loop(0, C // 8, body, 0)


def gates(zh, m, wt, bp, scr_a, scr_b, g_ref, r):
    p = dot(wt[...], zh)
    put_row(scr_a, r, sig(p[0:C] + bp[0]) * (p[C:N] + bp[1]) * m)
    put_row(scr_b, r, sig(p[N:384] + bp[2]) * (p[384:512] + bp[3]) * m)
    g_ref[r] = sig(p[512:CP] + bp[4])


def groups(body):
    lax.fori_loop(0, RB // GR, body, 0)


def halves(v):
    return v[:, :C] + v[:, C:]


CHUNKS = ((0, CP, (0, 1, 2, 3)), (CP, 512, (0, 2, 3, 1)), (1152, 512, (0, 3, 1, 2)))
GROWS = 1664


def coords():
    return lax.axis_index("dp"), lax.axis_index("dap")


def partner(k):
    dp, dap = coords()
    if k < 2:
        bit = lax.rem(dap // (1 << k), 2)
        return bit, (dp, dap + (1 << k) * (1 - 2 * bit))
    bit = lax.rem(dp // (1 << (k - 2)), 2)
    return bit, (dp + (1 << (k - 2)) * (1 - 2 * bit), dap)


def greet(keys):
    barrier = pltpu.get_barrier_semaphore()
    for k in keys:
        pl.semaphore_signal(barrier, inc=1, device_id=partner(k)[1], device_id_type=pl.DeviceIdType.MESH)
    pl.semaphore_wait(barrier, len(keys))


def remote(src, dst, send, recv, k):
    return pltpu.make_async_remote_copy(src_ref=src, dst_ref=dst, send_sem=send, recv_sem=recv, device_id=partner(k)[1], device_id_type=pl.DeviceIdType.MESH)


def rb(i):
    return lax.rem(i + 4 * partner(1)[0], 8)


def first4(i):
    return lax.min(i, 3)


def pair_parts(step, st, out, split):
    bit = partner(0)[0]
    slot = lax.rem(step, 2)
    dst = out.at[:, pl.ds(pl.multiple_of(bit * C + rb(step) * RB, RB), RB), :]
    mine = theirs = st.at[slot]
    if split:
        mine = st.at[slot, :, :, pl.ds(pl.multiple_of(bit * C, C), C)]
        theirs = st.at[slot, :, :, pl.ds(pl.multiple_of((1 - bit) * C, C), C)]
    return slot, dst, mine, theirs


def pair_here(step, st, out, sems, split):
    slot, dst, mine, _ = pair_parts(step, st, out, split)
    return pltpu.make_async_copy(mine, dst, sems[0].at[slot])


def pair_there(step, st, out, sems, split):
    slot, dst, _, theirs = pair_parts(step, st, out, split)
    return remote(theirs, dst, sems[1].at[slot], sems[2].at[step], 0)


def ship(step, items):
    @pl.when(step >= 2)
    def _():
        for _, *it in items:
            pair_here(step - 2, *it).wait()
            pair_there(step - 2, *it).wait_send()
    for scr, *it in items:
        pack(scr, it[0].at[lax.rem(step, 2)])
        pair_here(step, *it).start()
        pair_there(step, *it).start()

    @pl.when(step == 7)
    def _():
        for _, *it in items:
            for k in (6, 7):
                pair_here(k, *it).wait()
                pair_there(k, *it).wait_send()
            for k in range(8):
                pair_there(k, *it).wait_recv()


def ship_scratch():
    return [pltpu.VMEM((2, C, RB, N), BF16), pltpu.SemaphoreType.DMA((2,)), pltpu.SemaphoreType.DMA((2,)), pltpu.SemaphoreType.DMA((8,))]


def pre_kernel(z_ref, dz_ref, m_ref, lni_ref, lnm_ref, bo_ref, bproj_ref, wp_ref, wo_ref, a_ref, zh_ref, zt_ref, g_ref, mall_ref, prm_ref, wt_ref, wot_ref, af_ref, bf_ref, dzs_ref,
               scr_a, scr_b, dzbuf, dzsem, mbuf, zbuf, zloc, zsend, zrecv, msem, st_a, la, sa, ra, st_b, lb, sb, rb_):
    step = pl.program_id(0)
    xb = partner(1)[0]

    def z_here(q):
        return pltpu.make_async_copy(z_ref.at[pl.ds(q * RB, RB)], zbuf.at[pl.ds(q * RB, RB)], zloc.at[q])

    def z_there(q):
        return remote(z_ref.at[pl.ds(q * RB, RB)], zbuf.at[pl.ds(HB + q * RB, RB)], zsend.at[q], zrecv.at[q], 1)

    def dz_in():
        return pltpu.make_async_copy(dz_ref.at[pl.ds(0, DZ1)], dzbuf, dzsem.at[0])

    def dz_out():
        return pltpu.make_async_copy(dzbuf, dzs_ref, dzsem.at[1])

    @pl.when(step == 1)
    def _():
        dz_in().start()

    @pl.when(step == 3)
    def _():
        dz_in().wait()
        dz_out().start()

    @pl.when(step == 6)
    def _():
        dz_out().wait()

    m_dst = mbuf.at[pl.ds(pl.multiple_of(xb * HB, HB), HB), :]

    def m_there():
        return remote(m_dst, m_dst, msem.at[1], msem.at[2], 1)

    @pl.when(step == 0)
    def _():
        for q in range(4):
            z_here(q).start()
        m_dst[...] = by_chip(m_ref[...].astype(F32))
        greet((0, 1))
        m_there().start()
        for q in range(4):
            z_there(q).start()
        for k in range(2):
            vecs = [ref[k, q:q + 1].astype(F32) for ref in (lni_ref, lnm_ref) for q in range(2)] + [bo_ref[k:k + 1].astype(F32)]
            vecs += [bproj_ref[k:k + 1, q * C:q * C + C].astype(F32) for q in range(5)]
            cols = jnp.transpose(jnp.concatenate(vecs + [jnp.zeros((6, C), F32)], axis=0))
            for q in range(10):
                prm_ref[k, q] = jnp.broadcast_to(cols[:, q:q + 1], (C, N))
            wt_ref[k] = jnp.transpose(wp_ref[k])
            wot_ref[k] = jnp.transpose(wo_ref[k])
    for q in range(4):
        @pl.when(step == q)
        def _():
            z_here(q).wait()

        @pl.when(step == 4 + q)
        def _():
            if q == 0:
                m_there().wait()
            z_there(q).wait()

    def row(r, _):
        zt = load_t(zbuf, step * RB + r)
        zt_ref[r] = zt.astype(BF16)
        zn, _ = norm(zt)
        zh = (zn * prm_ref[0, 0] + prm_ref[0, 1]).astype(BF16)
        zh_ref[r] = zh
        gates(zh, mbuf[pl.ds(rb(step) * RB + r, 1), :], wt_ref.at[0], prm_ref.at[0, 5:10], scr_a, scr_b, g_ref, r)
        return 0
    lax.fori_loop(0, RB, row, 0, unroll=UN)
    ship(step, [(scr_a, st_a, af_ref, (la, sa, ra), False), (scr_b, st_b, bf_ref, (lb, sb, rb_), False)])
    a_ref[...] = st_a[lax.rem(step, 2)]

    @pl.when(step == 7)
    def _():
        mall_ref[...] = mbuf[...]


def mid_kernel(x_ref, g_ref, zt_ref, m_ref, lnm_ref, wot_ref, bo_ref, ln_ref, wt_ref, bp_ref,
               zm_ref, zh1_ref, g1_ref, ao_ref, bo1_ref, ac_ref, bf_ref, scr_x, scr_a, scr_b, st_a, la, sa, ra, st_b, lb, sb, rb_):
    step = pl.program_id(0)

    @pl.when(step == 0)
    def _():
        greet((0,))
    unpack(x_ref, scr_x)

    def row(r, _):
        xn, _ = norm(get_row(scr_x, r))
        xh = (xn * lnm_ref[0] + lnm_ref[1]).astype(BF16)
        u = dot(wot_ref[...], xh) + bo_ref[...]
        zm = (zt_ref[r].astype(F32) + g_ref[r] * u).astype(BF16)
        zm_ref[r] = zm
        zn, _ = norm(zm.astype(F32))
        zh = (zn * ln_ref[0] + ln_ref[1]).astype(BF16)
        zh1_ref[r] = zh
        gates(zh, m_ref[pl.ds(r, 1), :], wt_ref, bp_ref, scr_a, scr_b, g1_ref, r)
        return 0
    lax.fori_loop(0, RB, row, 0, unroll=UN)
    ship(step, [(scr_a, st_a, ac_ref, (la, sa, ra), True), (scr_b, st_b, bf_ref, (lb, sb, rb_), False)])

    @pl.when(step < 4)
    def _():
        ao_ref[...] = st_a[lax.rem(step, 2)]
        bo1_ref[...] = st_b[lax.rem(step, 2)]


def post_row(x, g, lnm_ref, wot_ref, wo_ref, bo_ref, dz):
    xn, rstd = norm(x)
    xh = (xn * lnm_ref[0] + lnm_ref[1]).astype(BF16)
    u = dot(wot_ref[...], xh) + bo_ref[...]
    d_pg = dz * u * (g * (1.0 - g))
    d_upd = dz * g
    d_bf = d_upd.astype(BF16)
    d_xh = dot(wo_ref[...], d_bf)
    dx = norm_bwd(d_xh, xn, rstd, lnm_ref[0])
    return xh, xn, u, d_pg, d_upd, d_bf, d_xh, dx


def post_vecs(vec_ref, d_upd, d_xh, xn, d_pg):
    for q, v in enumerate((d_upd, d_xh * xn, d_xh, d_pg)):
        vec_ref[q] += halves(v)


def add_outer(acc_ref, left, right):
    acc_ref[...] += dot(jnp.concatenate(left, axis=1), jnp.transpose(jnp.concatenate(right, axis=1)))


def zero(*refs):
    for ref in refs:
        ref[...] = jnp.zeros_like(ref)


def post1_kernel(x_ref, g_ref, zm_ref, dz_ref, dzo_ref, dzall_ref, lnm_ref, wot_ref, wo_ref, bo_ref,
                 zo_ref, dpg_ref, dzt_ref, dwo_ref, vec_ref, dxf_ref, scr_x, scr_d, dzbuf, dzsem, st, lsem, ssem, rsem):
    step = pl.program_id(0)

    def dz_there():
        return remote(dzall_ref.at[pl.ds(DZ1, RB)], dzbuf.at[1], dzsem.at[0], dzsem.at[1], 1)

    @pl.when(step == 0)
    def _():
        greet((0, 1))
        dz_there().start()
        zero(dwo_ref, vec_ref)
    unpack(x_ref, scr_x)

    @pl.when((step >= 4) & (step < 7))
    def _():
        def copy_row(r, _):
            dzbuf[0, r] = dzo_ref[r]
            return 0
        lax.fori_loop(0, RB, copy_row, 0)

    @pl.when(step == 7)
    def _():
        dz_there().wait()

    @pl.when(step >= 4)
    def _():
        def row(r, _):
            dz = load_t(dzbuf.at[step // 7], r)
            res = post_row(get_row(scr_x, r), g_ref[r], lnm_ref, wot_ref, wo_ref, bo_ref, dz)
            put_row(scr_d, r, res[-1])
            return 0
        lax.fori_loop(0, RB, row, 0, unroll=GR)

    @pl.when(step < 4)
    def _():
        def group(i, _):
            left, right = [], []
            for k in range(GR):
                r = i * GR + k
                dz = load_t(dz_ref, r)
                dzt_ref[r] = dz.astype(BF16)
                g = g_ref[r]
                xh, xn, u, d_pg, d_upd, d_bf, d_xh, dx = post_row(get_row(scr_x, r), g, lnm_ref, wot_ref, wo_ref, bo_ref, dz)
                put_row(scr_d, r, dx)
                dpg_ref[r] = d_pg.astype(BF16)
                zo_ref[r] = (zm_ref[r].astype(F32) + g * u).astype(BF16)
                post_vecs(vec_ref, d_upd, d_xh, xn, d_pg)
                left.append(xh)
                right.append(d_bf)
            add_outer(dwo_ref, left, right)
            return 0
        groups(group)
    ship(step, [(scr_d, st, dxf_ref, (lsem, ssem, rsem), False)])


def pre_bwd_row(r, k, z, zh, m, d_pg, scr_a, scr_b, ln_ref, wt_ref, w_ref, bp_ref, dp_ref, vec_ref):
    p = dot(wt_ref[0:512, :], zh)
    cols = slice(k * N, k * N + N)
    for q, scr in ((0, scr_a), (1, scr_b)):
        s = sig(p[q * N:q * N + C] + bp_ref[2 * q])
        v = p[q * N + C:q * N + N] + bp_ref[2 * q + 1]
        d_s = get_row(scr, r) * m
        d_v = d_s * s
        d_g = d_v * v * (1.0 - s)
        dp_ref[q * N:q * N + C, cols] = d_g.astype(BF16)
        dp_ref[q * N + C:q * N + N, cols] = d_v.astype(BF16)
        vec_ref[2 * q] += halves(d_g)
        vec_ref[2 * q + 1] += halves(d_v)
    dp_ref[512:CP, cols] = d_pg
    d_zh = dot(w_ref[...], dp_ref[:, cols])
    zn, rstd = norm(z)
    vec_ref[4] += halves(d_zh * zn)
    vec_ref[5] += halves(d_zh)
    return norm_bwd(d_zh, zn, rstd, ln_ref[0])


def midb_kernel(da_ref, db_ref, zh1_ref, zm_ref, m_ref, dpg1_ref, dzt_ref, x0_ref, g0_ref,
                ln_ref, wt_ref, w_ref, bp_ref, lnm_ref, wot_ref, wo_ref, bo_ref,
                dzm_ref, dx_ref, dpg0_ref, dwp_ref, dwo_ref, vec_ref, vec2_ref, dxk_ref, scr_a, scr_b, scr_x, scr_d, dp_ref,
                scr_e, st, lsem, csend, crecv, xsend, xrecv, rsend, rrecv):
    step = pl.program_id(0)
    cbit = partner(0)[0]
    xbit = partner(1)[0]

    def block(core, chip, k):
        return dxk_ref.at[:, pl.ds(pl.multiple_of(core * C + chip * HB + k * RB, RB), RB), :]

    def part(k, chip):
        return st.at[lax.rem(k, 2), :, :, pl.ds(pl.multiple_of(chip * C, C), C)]

    def here(k):
        return pltpu.make_async_copy(part(k, xbit), block(cbit, xbit, k), lsem.at[lax.rem(k, 2)])

    def to_core(k):
        return remote(part(k, xbit), block(cbit, xbit, k), csend.at[lax.rem(k, 2)], crecv.at[k], 0)

    def to_chip(k):
        return remote(part(k, 1 - xbit), block(cbit, xbit, k), xsend.at[lax.rem(k, 2)], xrecv.at[k], 1)

    def relay(k):
        blk = block(cbit, 1 - xbit, k)
        return remote(blk, blk, rsend.at[k], rrecv.at[k], 0)

    def settle(k):
        here(k).wait()
        to_core(k).wait_send()
        to_chip(k).wait_send()

    @pl.when(step == 0)
    def _():
        greet((0, 1))
        zero(dwp_ref, dwo_ref, vec_ref, vec2_ref)
    unpack(da_ref, scr_a)
    unpack(db_ref, scr_b)
    unpack(x0_ref, scr_x)

    def group(i, _):
        left, right, zhs = [], [], []
        for k in range(GR):
            r = i * GR + k
            zh = zh1_ref[r]
            zhs.append(zh)
            dz_norm = pre_bwd_row(r, k, zm_ref[r].astype(F32), zh, m_ref[pl.ds(r, 1), :], dpg1_ref[r], scr_a, scr_b,
                                  ln_ref, wt_ref, w_ref, bp_ref, dp_ref, vec_ref)
            dzm = (dzt_ref[r].astype(F32) + dz_norm).astype(BF16)
            dzm_ref[r] = dzm
            xh, xn, u, d_pg, d_upd, d_bf, d_xh, dx = post_row(get_row(scr_x, r), g0_ref[r], lnm_ref, wot_ref, wo_ref, bo_ref, dzm.astype(F32))
            put_row(scr_d, r, dx)
            put_row(scr_e, r, by_chip(dx))
            dpg0_ref[r] = d_pg.astype(BF16)
            post_vecs(vec2_ref, d_upd, d_xh, xn, d_pg)
            left.append(xh)
            right.append(d_bf)
        add_outer(dwo_ref, left, right)
        add_outer(dwp_ref, [dp_ref[...]], zhs)
        return 0
    groups(group)

    @pl.when(step >= 2)
    def _():
        settle(step - 2)
    pack(scr_e, st.at[lax.rem(step, 2)])
    to_chip(step).start()
    to_core(step).start()
    here(step).start()
    pack(scr_d, dx_ref)

    @pl.when(step >= 2)
    def _():
        to_chip(step - 2).wait_recv()
        relay(step - 2).start()

    @pl.when(step == 3)
    def _():
        for k in (2, 3):
            to_chip(k).wait_recv()
            relay(k).start()
            settle(k)
        for k in range(4):
            to_core(k).wait_recv()
            relay(k).wait()


def last_kernel(da_ref, db_ref, zh_ref, zt_ref, m_ref, dpg_ref, dzm_ref, zo_ref, ln_ref, wt_ref, w_ref, bp_ref,
                dz_ref, zout_ref, dwp_ref, vec_ref, scr_a, scr_b, dp_ref):
    @pl.when(pl.program_id(0) == 0)
    def _():
        zero(dwp_ref, vec_ref)
    unpack(da_ref, scr_a)
    unpack(db_ref, scr_b)

    def group(i, _):
        zhs = []
        for k in range(GR):
            r = i * GR + k
            zh = zh_ref[r]
            zhs.append(zh)
            dz_norm = pre_bwd_row(r, k, zt_ref[r].astype(F32), zh, m_ref[pl.ds(r, 1), :], dpg_ref[r], scr_a, scr_b,
                                  ln_ref, wt_ref, w_ref, bp_ref, dp_ref, vec_ref)
            store_t(dz_ref, r, (dzm_ref[r].astype(F32) + dz_norm).astype(BF16))
            store_t(zout_ref, r, zo_ref[r])
        add_outer(dwp_ref, [dp_ref[...]], zhs)
        return 0
    groups(group)


def grads1_kernel(a_ref, b_ref, dx_ref, da_ref, db_ref):
    for k in range(CB):
        dx = dx_ref[k]
        da_ref[k] = dot(b_ref[k], jnp.transpose(dx)).astype(BF16)
        db_ref[k] = dot(a_ref[k], dx).astype(BF16)


def grads0_kernel(dx_ref, b_ref, dxk_ref, a_ref, da_ref, db_ref, turned):
    own = pl.ds(pl.multiple_of(partner(0)[0] * HB, HB), HB)
    for k in range(CB):
        turned[k] = jnp.transpose(dxk_ref[k])
        da_ref[k] = dot(dx_ref[k], b_ref[k]).astype(BF16)
    for k in range(CB):
        db_ref[k] = dot(turned[k, own, :], a_ref[k]).astype(BF16)


def sds(shape, dtype):
    return jax.ShapeDtypeStruct(shape, dtype)


def full(shape):
    nd = len(shape)
    return pl.BlockSpec(shape, lambda *_: (0,) * nd)


def rows_spec(shape, fn):
    return pl.BlockSpec((RB,) + shape, lambda i: (fn(i),) + (0,) * len(shape))


def cm_spec(fn):
    return pl.BlockSpec((C, RB, N), lambda i: (0, fn(i), 0))


def scr():
    return pltpu.VMEM((2, C * SP, C), F32)


ANY = pl.BlockSpec(memory_space=pl.ANY)


def call(kernel, grid, in_specs, out_specs, out_shape, scratch, name, cid=None):
    return pl.pallas_call(
        kernel, name=name, out_shape=out_shape, grid=(grid,), in_specs=in_specs, out_specs=out_specs, scratch_shapes=scratch,
        compiler_params=pltpu.CompilerParams(dimension_semantics=("arbitrary",), vmem_limit_bytes=60 << 20, collective_id=cid, has_side_effects=cid is not None))


def reduce_kernel(dwp0_ref, dwo0_ref, pre0_ref, post0_ref, dwp1_ref, dwo1_ref, pre1_ref, post1_ref, out_ref, acc, got0, got1, got2, got3, send, recv):
    greet((0, 1, 2, 3))
    parts = ((dwp0_ref, dwo0_ref, pre0_ref, post0_ref), (dwp1_ref, dwo1_ref, pre1_ref, post1_ref))
    for k, (dwp, dwo, vpre, vpost) in enumerate(parts):
        acc[784 * k:784 * k + CP, :] = dwp[...]
        acc[784 * k + CP:784 * k + 768, :] = dwo[...]
        rows = [jnp.sum(jnp.transpose(v[q]), axis=0, keepdims=True) for v, n in ((vpre, 6), (vpost, 4)) for q in range(n)]
        acc[784 * k + 768:784 * k + 784, :] = jnp.concatenate(rows + [jnp.zeros((6, C), F32)], axis=0)
    acc[1568:GROWS, :] = jnp.zeros((GROWS - 1568, C), F32)
    got = (got0, got1, got2, got3)
    spans = [[r0, n] for r0, n, _ in CHUNKS]
    for st in range(4):
        copies = []
        base = 0
        for ch, (_, _, order) in enumerate(CHUNKS):
            lo, n = spans[ch]
            half = n // 2
            bit = partner(order[st])[0]
            give = pl.multiple_of(lo + (1 - bit) * half, 8)
            keep = pl.multiple_of(lo + bit * half, 8)
            land = got[st].at[pl.ds(base, half), :]
            cp = remote(acc.at[pl.ds(give, half), :], land, send.at[st, ch], recv.at[st, ch], order[st])
            cp.start()
            copies.append((cp, keep, half, base))
            spans[ch] = [keep, half]
            base += half
        for cp, keep, half, base in copies:
            cp.wait()
            acc[pl.ds(keep, half), :] += got[st][base:base + half, :]
    for lo, n in spans:
        out_ref[pl.ds(lo, n), :] = acc[pl.ds(lo, n), :]
    for st in (3, 2, 1, 0):
        copies = []
        for ch, (_, _, order) in enumerate(CHUNKS):
            lo, n = spans[ch]
            bit = partner(order[st])[0]
            seg = out_ref.at[pl.ds(pl.multiple_of(lo, 8), n), :]
            cp = remote(seg, seg, send.at[4 + st, ch], recv.at[4 + st, ch], order[st])
            cp.start()
            copies.append(cp)
            spans[ch] = [lo - bit * n, 2 * n]
        for cp in copies:
            cp.wait()


def reduce_all(*g):
    vm = pl.BlockSpec(memory_space=pltpu.VMEM)
    return pl.pallas_call(
        reduce_kernel, name="reduce", out_shape=sds((GROWS, C), F32), in_specs=[vm] * 8, out_specs=vm,
        scratch_shapes=[pltpu.VMEM((GROWS, C), F32)] + [pltpu.VMEM((GROWS >> (k + 1), C), F32) for k in range(4)]
        + [pltpu.SemaphoreType.DMA((8, 3)), pltpu.SemaphoreType.DMA((8, 3))],
        compiler_params=pltpu.CompilerParams(collective_id=0, has_side_effects=True))(*g)


def solution(mesh):
    def local_step(z_pair, pair_mask, dz_out, ln_in, w_proj, b_proj, ln_mid, w_out, b_out):
        def pick(k, *shape):
            return pl.BlockSpec((None,) + shape, lambda i: (k,) + (0,) * len(shape))

        def vecs(k, n, at):
            return pl.BlockSpec((None, n, C, N), lambda i: (k, at, 0, 0))

        def ln_s(k):
            return [vecs(k, 2, 0)]

        def mid_s(k):
            return [vecs(k, 2, 1)]

        def bias_s(k):
            return [pl.BlockSpec((None, None, C, N), lambda i: (k, 4, 0, 0))]

        def proj_s(k):
            return [pick(k, CP, C)]

        def bp_s(k):
            return [vecs(k, 5, 1)]

        same = lambda i: i
        cm_all = sds((C, C, N), BF16)
        cm_full = sds((C, N, N), BF16)
        cm_own = sds((C, HB, N), BF16)
        rt_all = sds((C, C, N), BF16)
        rt_f32 = sds((C, C, N), F32)
        rt_own = sds((HB, C, N), BF16)
        vm = pl.BlockSpec(memory_space=pltpu.VMEM)

        a0, zh0, zt0, g0, mask_all, prm, wt, wot, a0f, b0f, dz_head = call(
            pre_kernel, 8, [ANY, ANY] + [vm] * 7,
            [cm_spec(rb), rows_spec((C, N), rb), rows_spec((C, N), rb), rows_spec((C, N), rb), vm, vm, vm, vm, ANY, ANY, ANY],
            [cm_all, rt_all, rt_all, rt_f32, sds((C, N), F32), sds((2, 10, C, N), F32), sds((2, CP, C), BF16), sds((2, C, C), BF16), cm_full, cm_full, sds((DZ1, N, C), BF16)],
            [scr(), scr(), pltpu.VMEM((DZ1, N, C), BF16), pltpu.SemaphoreType.DMA((2,)), pltpu.VMEM((C, N), F32), pltpu.VMEM((C, N, C), BF16)] + [pltpu.SemaphoreType.DMA((4,))] * 3 + [pltpu.SemaphoreType.DMA((3,))] + ship_scratch() * 2,
            "pre", 1)(z_pair[0], dz_out[0], pair_mask[0], ln_in, ln_mid, b_out, b_proj, w_proj, w_out)
        dz_own = dz_out[0]
        dz_oth = lax.ppermute(dz_head, "dap", SWAP_X)
        x0 = jnp.einsum("cik,cjk->cij", a0, b0f, preferred_element_type=F32)

        zm, zh1, g1, a1o, b1o, a1c, b1f = call(
            mid_kernel, 8,
            [cm_spec(rb), rows_spec((C, N), rb), rows_spec((C, N), rb), rows_spec((N,), rb)] + mid_s(0) + [pick(0, C, C)] + bias_s(0) + ln_s(1) + proj_s(1) + bp_s(1),
            [rows_spec((C, N), rb), rows_spec((C, N), rb), rows_spec((C, N), rb), cm_spec(first4), cm_spec(first4), ANY, ANY],
            [rt_all, rt_all, rt_f32, cm_own, cm_own, sds((C, N, C), BF16), cm_full],
            [scr(), scr(), scr()] + ship_scratch() * 2,
            "mid", 2)(x0, g0, zt0, mask_all, prm, wot, prm, prm, wt, prm)
        x1 = jnp.einsum("cki,ckj->cij", a1c, b1f, preferred_element_type=F32)

        late = lambda i: lax.min(lax.max(i - 4, 0), 2)
        smb = lambda k: mid_s(k) + [pick(k, C, C), pick(k, C, C)] + bias_s(k)
        zo, dpg1, dzt, dwo1, vec1, dx1f = call(
            post1_kernel, 8,
            [cm_spec(rb), rows_spec((C, N), rb), rows_spec((C, N), rb), rows_spec((N, C), first4), rows_spec((N, C), late), ANY] + smb(1),
            [rows_spec((C, N), first4), rows_spec((C, N), first4), rows_spec((C, N), first4), full((C, C)), full((4, C, C)), ANY],
            [rt_own, rt_own, rt_own, sds((C, C), F32), sds((4, C, C), F32), cm_full],
            [scr(), scr(), pltpu.VMEM((2, RB, N, C), BF16), pltpu.SemaphoreType.DMA((2,))] + ship_scratch(), "post1", 3)(
            x1, g1, zm, dz_own, dz_oth, dz_own, prm, wot, w_out, prm)
        chan = lambda *sh: pl.BlockSpec((CB,) + sh, lambda i: (i, 0, 0))
        da1, db1 = call(grads1_kernel, C // CB, [chan(HB, N), chan(HB, N), chan(N, N)], [chan(HB, N)] * 2, [cm_own] * 2, [], "grads1")(a1o, b1o, dx1f)

        own = lambda i: i + 4 * partner(1)[0]
        wp = lambda k: ln_s(k) + proj_s(k) + [pick(k, C, CP)] + bp_s(k)
        dzm, dx0, dpg0, dwp1, dwo0, vec2, vec3, dx0k = call(
            midb_kernel, 4,
            [cm_spec(same), cm_spec(same), rows_spec((C, N), own), rows_spec((C, N), own), rows_spec((N,), own),
             rows_spec((C, N), same), rows_spec((C, N), same), cm_spec(own), rows_spec((C, N), own)] + wp(1) + smb(0),
            [rows_spec((C, N), same), cm_spec(same), rows_spec((C, N), same), full((CP, C)), full((C, C)), full((6, C, C)), full((4, C, C)), ANY],
            [rt_own, sds((C, HB, N), BF16), rt_own, sds((CP, C), F32), sds((C, C), F32), sds((6, C, C), F32), sds((4, C, C), F32), sds((C, N, C), BF16)],
            [scr(), scr(), scr(), scr(), pltpu.VMEM((CP, GR * N), BF16), scr(), pltpu.VMEM((2, C, RB, N), BF16)]
            + [pltpu.SemaphoreType.DMA((k,)) for k in (2, 2, 4, 2, 4, 4, 4)], "midb", 4)(
            da1, db1, zh1, zm, mask_all, dpg1, dzt, x0, g0, prm, wt, w_proj, prm,
            prm, wot, w_out, prm)
        da0, db0 = call(grads0_kernel, C // CB, [chan(HB, N), chan(N, N), chan(N, C), chan(N, N)], [chan(HB, N)] * 2, [cm_own] * 2,
                        [pltpu.VMEM((CB, C, N), BF16)], "grads0")(dx0, b0f, dx0k, a0f)

        dzp, zo, dwp0, vec4 = call(
            last_kernel, 4,
            [cm_spec(same), cm_spec(same), rows_spec((C, N), own), rows_spec((C, N), own), rows_spec((N,), own),
             rows_spec((C, N), same), rows_spec((C, N), same), rows_spec((C, N), same)] + wp(0),
            [rows_spec((N, C), same), rows_spec((N, C), same), full((CP, C)), full((6, C, C))],
            [sds((HB, N, C), BF16), sds((HB, N, C), BF16), sds((CP, C), F32), sds((6, C, C), F32)],
            [scr(), scr(), pltpu.VMEM((CP, GR * N), BF16)], "last")(
            da0, db0, zh0, zt0, mask_all, dpg0, dzm, zo, prm, wt, w_proj, prm)

        g = reduce_all(dwp0, dwo0, vec4, vec3, dwp1, dwo1, vec2, vec1)[:1568].reshape(2, 784, C)
        d_b = jnp.concatenate([g[:, 768:772].reshape(2, 512), g[:, 777]], axis=1)
        return (zo[None], dzp[None], g[:, 772:774], jnp.swapaxes(g[:, :CP], 1, 2), d_b, g[:, 775:777], g[:, CP:768], g[:, 774])

    row_spec = P("dp", "dap")
    return jax.shard_map(local_step, mesh=mesh, in_specs=(row_spec, row_spec, row_spec, P(), P(), P(), P(), P(), P()), out_specs=(row_spec, row_spec, P(), P(), P(), P(), P(), P()), check_vma=False)
```
